256 devices in a mesh: shot: 64 (over y, z, core), grp: 4 (over x).
Axes of the slice: x: 4, y: 4, z: 8, core: 2. Of those that a mesh axis runs over, the one named last changes fastest.
Arguments:
- offsets: bfloat16 [49152, 32, 512], P(('shot', 'grp')), may hold values from -500 to 500
- slant_weights: bfloat16 [64, 32], replicated, may hold values from -1 to 1
- live: int32 [49152, 64], P(('shot', 'grp')), may hold values from 0 to 1, as said below
- block_tile: int32 [24576, 1], P(('shot', 'grp')), may hold values from 0 to 63; in each aligned block of 96 rows (0 to 95, 96 to 191, ...) at most 2 rows name the same one
- image_slot: int32 [24576], P(('shot', 'grp')), may hold values from 0 to 15
Outputs:
- image: bfloat16 [1024, 128, 512], P(('shot', 'grp'))
The draws below stay inside these ranges and needn't reach their ends.
Inputs may be any that keep to these rules, and one draw needn't show every extreme that they name: Each position's live angles are 0 up to a cutoff minus 1, the cutoff at least 16; the first position of every 192 positions keeps all 64 angles. `block_tile`: among the 96 blocks of one device no tile is named more than 2 times.
All inputs are finite; a program needn't handle non-finite values.
Results may differ from the reference program's by a relative error of at most 0.0049.
Values may be sent and summed in bfloat16 or wider, within the bound.
No kernel may reach another device: no remote copies, remote signals or barrier semaphores. Data moves between devices by JAX's collectives and lax.ppermute only.
A program may use at most 192 MiB of HBM per device.

```python
import math
import jax
import jax.numpy as jnp
import numpy as np
from jax import lax

ANG = 64
H = 32
Z = 512
TRB = 128
BLK_DEV = 96
IMG_DEV = 4
CAP = 2
POS_DEV = 192
POSITIONS = 49152
BLOCKS = 24576
IT = 16
IMAGE_BLOCKS = 1024
N_SHOT = 64
N_GRP = 4
DEVICES = 256


def draw_offsets(key, part):
    keys = jax.random.split(jax.random.fold_in(key, 11), 3)
    row_scale = jnp.exp(jax.random.uniform(keys[1], (POSITIONS, 1, 1), jnp.float32) * jnp.log(10.0))
    depth_scale = jnp.exp(jax.random.uniform(keys[2], (1, 1, Z), jnp.float32) * jnp.log(10.0))
    place = jnp.arange(POSITIONS, dtype=jnp.float32) / max(POSITIONS - 1, 1)
    base = jnp.clip(jax.random.normal(keys[0], (POSITIONS, H, Z), jnp.float32), -6.0, 6.0)
    ramp = 1.0 + 2.0 * place
    values = 0.1 * base * row_scale * depth_scale * ramp[:, None, None]
    return values.astype(jnp.bfloat16)


def draw_live(key, part):
    cutoff = jax.random.randint(jax.random.fold_in(key, 23), (POSITIONS,), ANG // 4, ANG + 1)
    first = jnp.arange(POSITIONS) % POS_DEV == 0
    cutoff = jnp.where(first, ANG, cutoff)
    return (jnp.arange(ANG)[None, :] < cutoff[:, None]).astype(jnp.int32)


def place_ends(drawn, key, low, top_value):
    spot = [jax.random.randint(jax.random.fold_in(key, axis), (), 0, length) for axis, length in enumerate(drawn.shape)]
    longest = drawn.shape.index(max(drawn.shape))
    next_to = spot[:longest] + [(spot[longest] + 1) % drawn.shape[longest]] + spot[longest + 1:]
    return drawn.at[tuple(spot)].set(low).at[tuple(next_to)].set(top_value)


def deal_out(key, own, number, rows, number_of, top, most, lean):
    order = jax.random.permutation(key, number_of)
    crowded, usual = shares(number_of, rows * top, most, lean, True), shares(number_of, rows * top, most, lean, False)
    places = jnp.arange(number_of)

    def named(lengths, rotation):
        used = int((lengths > 0).sum())
        fixed = max(1, used // 4)
        moved = fixed + (places - fixed + rotation * (used - fixed)) % max(1, number_of - fixed)
        return jnp.zeros((number_of,), jnp.int32).at[order[jnp.where(places < fixed, places, moved)]].set(jnp.asarray(lengths, jnp.int32))

    lengths = jnp.where(number % 4 == 0, named(crowded, number // 4), named(usual, number - number // 4 - 1))
    mixed = jax.random.permutation(jax.random.fold_in(own, 3), number_of)
    giver, receiver = mixed[0:number_of // 2 * 2:2], mixed[1:number_of // 2 * 2:2]
    margin = jnp.minimum(lengths[giver] - 1, most - lengths[receiver]) // 2
    margin = jnp.where((giver == order[0]) | (receiver == order[0]) | (lengths[receiver] == 0), 0, jnp.maximum(margin, 0))
    moved = jax.random.randint(jax.random.fold_in(own, 4), (number_of // 2,), 0, 1 << 20) % (margin + 1)
    lengths = lengths.at[giver].add(-moved).at[receiver].add(moved)
    labels = jnp.searchsorted(jnp.cumsum(lengths), jnp.arange(rows * top), side="right").astype(jnp.int32)
    table = labels.reshape(top, rows).T
    table = table[jax.random.permutation(jax.random.fold_in(own, 1), rows)]
    rotation = jax.random.randint(jax.random.fold_in(own, 2), (rows, 1), 0, top)
    return jnp.take_along_axis(table, (jnp.arange(top)[None, :] + rotation) % top, axis=1)


def shares(number_of, total, reach, lean, full):
    weights = [(1 << 20) // math.isqrt(standing ** lean) + 1 for standing in range(1, number_of + 1)]
    largest = reach if full else min(reach, max(-(-total // number_of), total * weights[0] // sum(weights)))
    least = 1 if total - largest >= number_of - 1 else 0
    counts, spare = [largest] + [least] * (number_of - 1), total - largest - least * (number_of - 1)
    while spare > 0:
        movable = [i for i in range(1, number_of) if counts[i] < largest] or [i for i in range(1, number_of) if counts[i] < reach]
        mass, budget = sum([weights[i] for i in movable]), spare
        for i in movable:
            more = min(reach - counts[i], max(1, budget * weights[i] // mass), spare)
            counts[i] = counts[i] + more
            spare = spare - more
    return np.array(counts)


def noise(rng, shape, width, most, kind=jnp.bfloat16):
    return jnp.clip(width * jax.random.normal(rng, shape, jnp.float32), -most, most).astype(kind)


def setup_inputs(seed: int = 0) -> dict:
    key_list = jax.random.split(jax.random.key(seed), 6)
    offsets = draw_offsets(jax.random.fold_in(key_list[5], 71), 0)
    slant_weights = noise(key_list[1], (ANG, H), H ** -0.5, 1.0)
    live = draw_live(jax.random.fold_in(key_list[5], 71), 0)
    block_tile_keys = jax.random.split(jax.random.fold_in(key_list[3], 1), BLOCKS // BLK_DEV)
    block_tile_turns = jax.random.permutation(jax.random.fold_in(key_list[3], 3), BLOCKS // BLK_DEV)
    block_tile = jax.vmap(lambda own, number: deal_out(jax.random.fold_in(key_list[3], 2), own, number, BLK_DEV, N_SHOT, 1, CAP, 1))(block_tile_keys, block_tile_turns).reshape((BLOCKS, 1))
    image_slot = place_ends(jax.random.randint(key_list[4], (BLOCKS,), 0, IT), jax.random.fold_in(key_list[4], 1), 0, IT - 1).astype(jnp.int32)
    return {"offsets": offsets, "slant_weights": slant_weights, "live": live, "block_tile": block_tile, "image_slot": image_slot}


def reference(offsets, slant_weights, live, block_tile, image_slot):
    tile_rows = IMG_DEV * N_GRP
    weights = slant_weights.astype(jnp.float32)
    shards = (offsets.reshape(DEVICES, POS_DEV, H, Z), live.reshape(DEVICES, POS_DEV, ANG), block_tile.reshape(DEVICES, BLK_DEV), image_slot.reshape(DEVICES, BLK_DEV))

    def advance(state_in, pieces):
        stacked, square_sum, live_count = state_in
        shard_off, shard_live, shard_tile, shard_slot = pieces
        live_mask = shard_live.astype(jnp.float32)
        slanted = jnp.einsum('ah,phz->paz', weights, shard_off.astype(jnp.float32))
        angles = (slanted * live_mask[:, :, None]).astype(jnp.bfloat16)
        widened = angles.astype(jnp.float32)
        square_sum = square_sum + lax.optimization_barrier(jnp.sum(widened * widened, axis=(0, 2)))
        live_count = live_count + lax.optimization_barrier(jnp.sum(live_mask, axis=0))
        targets = (shard_tile.astype(jnp.int32) * tile_rows + shard_slot.astype(jnp.int32)).astype(jnp.int32)
        stacked = stacked.at[targets].add(widened.reshape(BLK_DEV, TRB, Z))
        return ((stacked, square_sum, live_count), None)
    initial = (jnp.zeros((IMAGE_BLOCKS, TRB, Z), jnp.float32), jnp.zeros((ANG,), jnp.float32), jnp.zeros((ANG,), jnp.float32))
    (stacked, square_sum, live_count), unused = lax.scan(advance, initial, shards)
    angle_gain = lax.rsqrt(square_sum / (Z * live_count) + 1e-06)
    trace_gain = jnp.tile(angle_gain, 2)
    return (stacked * trace_gain[None, :, None]).astype(jnp.bfloat16)
```

```python
import functools

import jax
import jax.numpy as jnp
from jax import lax
from jax.experimental import pallas as pl
from jax.experimental.pallas import tpu as pltpu
from jax.sharding import Mesh
from jax.sharding import PartitionSpec as P

SHOT_GRP = ("shot_0", "shot_1", "shot_2", "grp")
PLANE = ("shot_0", "shot_2", "grp")
LANES = 128
CAP = 2
GROUP = 8


def pack_kernel(
    parity, tile_ref, slot_ref, live_ref, off_ref, out_ref,
    data, zeros, meta, meta_low, count, in_sems, out_sem, meta_sem,
):
    blocks = off_ref.shape[0]
    hh = off_ref.shape[2]
    quarters = data.shape[0]
    tiles = count.shape[0]
    rows = meta.shape[1]
    parts = in_sems.shape[0]
    step = blocks // parts
    angles = live_ref.shape[1]

    def load(g, q):
        return pltpu.make_async_copy(
            off_ref.at[pl.ds(g * step, step), parity, :, pl.ds(q * LANES, LANES)],
            data.at[q, pl.ds(g * step, step)],
            in_sems.at[g],
        )

    for g in range(parts):
        for q in range(quarters):
            load(g, q).start()
    zeros[...] = jnp.zeros_like(zeros)
    meta[...] = jnp.zeros_like(meta)

    def clear(t, _):
        count[t] = 0
        return 0

    lax.fori_loop(0, tiles, clear, 0)

    def place(tile, rank):
        column = (tile // 16) * 2 + tile % 2
        return column, ((tile // 2) % 8) * CAP + rank

    def target(column, row):
        return out_ref.at[column, :, pl.ds(pl.multiple_of(row * hh, hh), hh), :]

    def send(b, _):
        tile = tile_ref[b]
        rank = count[tile]
        count[tile] = rank + 1
        column, row = place(tile, rank)
        pltpu.make_async_copy(data.at[:, b], target(column, row), out_sem).start()
        flags = live_ref[pl.ds(b * 2 + parity, 1), :].astype(jnp.float32)
        meta[column, pl.ds(row, 1), :angles] = flags * (slot_ref[b] + 1).astype(jnp.float32)
        return 0

    for g in range(parts):
        for q in range(quarters):
            load(g, q).wait()
        lax.fori_loop(g * step, (g + 1) * step, send, 0)

    def fill(tile, _):
        used = count[tile]
        for rank in range(CAP):
            column, row = place(tile, rank)

            @pl.when(used <= rank)
            def _():
                pltpu.make_async_copy(zeros, target(column, row), out_sem).start()
        return 0

    lax.fori_loop(0, tiles, fill, 0)
    meta_low[...] = meta[...].astype(jnp.bfloat16)

    def meta_copy(q):
        return pltpu.make_async_copy(
            meta_low, out_ref.at[:, q, pl.ds(rows * hh, rows), :], meta_sem
        )

    for q in range(quarters):
        meta_copy(q).start()
    whole = out_ref.at[:, :, pl.ds(0, rows * hh), :]
    pltpu.make_async_copy(whole, whole, out_sem).wait()
    for q in range(quarters):
        meta_copy(q).wait()


def pack(parity, tiles, slots, live, blocks, columns, quarters, tile_count):
    count, _, hh, depth = blocks.shape
    rows = tile_count // columns * CAP
    parts = 8
    any_space = pl.BlockSpec(memory_space=pl.ANY)
    smem = pl.BlockSpec(memory_space=pltpu.SMEM)
    return pl.pallas_call(
        functools.partial(pack_kernel, parity),
        out_shape=jax.ShapeDtypeStruct(
            (columns, quarters, rows * hh + rows, LANES), jnp.bfloat16
        ),
        in_specs=[smem, smem, pl.BlockSpec(memory_space=pltpu.VMEM), any_space],
        out_specs=any_space,
        scratch_shapes=[
            pltpu.VMEM((quarters, count, hh, LANES), jnp.bfloat16),
            pltpu.VMEM((quarters, hh, LANES), jnp.bfloat16),
            pltpu.VMEM((columns, rows, LANES), jnp.float32),
            pltpu.VMEM((columns, rows, LANES), jnp.bfloat16),
            pltpu.SMEM((tile_count,), jnp.int32),
            pltpu.SemaphoreType.DMA((parts,)),
            pltpu.SemaphoreType.DMA,
            pltpu.SemaphoreType.DMA,
        ],
        compiler_params=pltpu.CompilerParams(vmem_limit_bytes=16 * 2**20),
        cost_estimate=pl.CostEstimate(
            flops=8_000_000_000, bytes_accessed=7 * 2**20, transcendentals=0
        ),
        name=f"pack{parity}",
    )(tiles, slots, live, blocks)


def stack_kernel(code_ref, w_ref, in_ref, out_ref, acc):
    step = pl.program_id(0)
    angles, lanes = acc.shape[2:]
    tile_rows = out_ref.shape[1]
    depth = w_ref.shape[1]
    slots = (in_ref.shape[1] * GROUP) // (depth + GROUP)

    @pl.when(step == 0)
    def _():
        acc[...] = jnp.zeros_like(acc)

    row = lax.broadcasted_iota(jnp.int32, (angles, lanes), 0)
    for u in range(in_ref.shape[0]):
        for part in range(slots // GROUP):
            product = jnp.dot(
                w_ref[...],
                in_ref[u, part * depth : (part + 1) * depth, :],
                preferred_element_type=jnp.float32,
            )
            for j in range(GROUP):
                slot = part * GROUP + j
                code = code_ref[(step * in_ref.shape[0] + u) * slots + slot]
                label = code // 128
                cut = code % 128
                angle = jnp.where(row < cut, product[j * angles : (j + 1) * angles], 0.0)
                acc[slot // CAP, label] += angle.astype(jnp.bfloat16).astype(jnp.float32)

    @pl.when(step == pl.num_programs(0) - 1)
    def _():
        out_ref[...] = acc[:, :tile_rows].astype(out_ref.dtype)


def stack(arrived, weights, tile_rows, hh):
    sources, length, lanes = arrived.shape
    slots = length // (hh + 1)
    angles = weights.shape[0] // GROUP
    flags = arrived[:, slots * hh :, :angles]
    label = jnp.max(flags, axis=2).astype(jnp.int32)
    cut = jnp.sum((flags > 0).astype(jnp.int32), axis=2)
    code = (jnp.where(label == 0, tile_rows, label - 1) * 128 + cut).reshape(-1)
    per = 4
    tiles = slots // CAP
    return pl.pallas_call(
        stack_kernel,
        grid=(sources // per,),
        out_shape=jax.ShapeDtypeStruct((tiles, tile_rows, angles, lanes), jnp.bfloat16),
        in_specs=[
            pl.BlockSpec(memory_space=pltpu.SMEM),
            pl.BlockSpec(weights.shape, lambda i: (0, 0)),
            pl.BlockSpec((per, length, lanes), lambda i: (i, 0, 0)),
        ],
        out_specs=pl.BlockSpec((tiles, tile_rows, angles, lanes), lambda i: (0, 0, 0, 0)),
        scratch_shapes=[pltpu.VMEM((tiles, tile_rows + 1, angles, lanes), jnp.float32)],
        compiler_params=pltpu.CompilerParams(vmem_limit_bytes=24 * 2**20),
        cost_estimate=pl.CostEstimate(
            flops=12_000_000_000, bytes_accessed=7 * 2**20, transcendentals=0
        ),
        name="stack",
    )(code, weights, arrived)


def moments_kernel(cut_ref, w_ref, in_ref, out_ref):
    step = pl.program_id(0)
    angles, lanes = out_ref.shape
    count, hh, depth = in_ref.shape

    @pl.when(step == 0)
    def _():
        out_ref[...] = jnp.zeros_like(out_ref)

    row = lax.broadcasted_iota(jnp.int32, (angles, lanes), 0)
    total = out_ref[...]
    for part in range(count // GROUP):
        gathers = in_ref[part * GROUP : (part + 1) * GROUP].reshape(GROUP * hh, depth)
        square = None
        for q in range(depth // lanes):
            product = jnp.dot(
                w_ref[...],
                gathers[:, q * lanes : (q + 1) * lanes],
                preferred_element_type=jnp.float32,
            )
            product = product.astype(jnp.bfloat16).astype(jnp.float32)
            square = product * product if square is None else square + product * product
        for j in range(GROUP):
            cut = cut_ref[step * count + part * GROUP + j]
            total += jnp.where(row < cut, square[j * angles : (j + 1) * angles], 0.0)
    out_ref[...] = total


def moments(offsets, weights, live):
    positions, hh, depth = offsets.shape
    angles = live.shape[1]
    per = 16
    squares = pl.pallas_call(
        moments_kernel,
        grid=(positions // per,),
        out_shape=jax.ShapeDtypeStruct((angles, LANES), jnp.float32),
        in_specs=[
            pl.BlockSpec(memory_space=pltpu.SMEM),
            pl.BlockSpec(weights.shape, lambda i: (0, 0)),
            pl.BlockSpec((per, hh, depth), lambda i: (i, 0, 0)),
        ],
        out_specs=pl.BlockSpec((angles, LANES), lambda i: (0, 0)),
        compiler_params=pltpu.CompilerParams(vmem_limit_bytes=24 * 2**20),
        cost_estimate=pl.CostEstimate(
            flops=12_000_000_000, bytes_accessed=6 * 2**20, transcendentals=0
        ),
        name="moments",
    )(jnp.sum(live, axis=1), weights, offsets)
    return jnp.sum(squares, axis=1), jnp.sum(live, axis=0).astype(jnp.float32)


def finish_kernel(gain_ref, first_ref, second_ref, out_ref):
    quarters, images, angles, lanes = first_ref.shape
    gain = gain_ref[...]
    for half, ref in enumerate((first_ref, second_ref)):
        for q in range(quarters):
            for k in range(images):
                value = ref[q, k].astype(jnp.float32) * gain
                out_ref[
                    k, half * angles : (half + 1) * angles, q * lanes : (q + 1) * lanes
                ] = value.astype(out_ref.dtype)


def finish(gain, first, second):
    quarters, images, angles, lanes = first.shape
    vmem = pl.BlockSpec(memory_space=pltpu.VMEM)
    return pl.pallas_call(
        finish_kernel,
        out_shape=jax.ShapeDtypeStruct((images, 2 * angles, quarters * lanes), jnp.bfloat16),
        in_specs=[vmem, vmem, vmem],
        out_specs=vmem,
        name="finish",
    )(jnp.broadcast_to(gain[:, None], (angles, lanes)), first, second)


def local(offsets, slant_weights, live, block_tile, image_slot):
    block_count = block_tile.shape[0]
    _, hh, depth = offsets.shape
    angles = slant_weights.shape[0]
    tile_count = lax.axis_size(("shot_0", "shot_1", "shot_2"))
    columns = lax.axis_size(("shot_0", "shot_2"))
    quarters = lax.axis_size("grp")
    tile_rows = 4 * quarters
    blocks = offsets.reshape(block_count, 2, hh, depth)
    tiles = block_tile[:, 0]
    weights = jnp.kron(jnp.eye(GROUP, dtype=jnp.bfloat16), slant_weights)

    ends = []
    for parity in range(2):
        sent = pack(
            parity, tiles, image_slot, live, blocks, columns, quarters, tile_count
        )
        sent = sent.reshape((columns * quarters,) + sent.shape[2:])
        arrived = lax.all_to_all(sent, PLANE, 0, 0, tiled=True)
        dense = stack(arrived, weights, tile_rows, hh)
        dense = dense.reshape((-1, angles, LANES))
        summed = lax.psum_scatter(dense, "shot_1", scatter_dimension=0, tiled=True)
        swapped = summed.reshape(quarters, 4, angles, LANES)
        ends.append(lax.all_to_all(swapped, "grp", 0, 0, tiled=True))

    squares, counts = moments(offsets, weights, live)
    totals = lax.psum(jnp.concatenate([squares, counts]), SHOT_GRP)
    gain = lax.rsqrt(totals[:angles] / (depth * totals[angles:]) + 1e-06)
    return finish(gain, ends[0], ends[1])


def solution(mesh):
    torus = Mesh(
        mesh.devices.reshape(4, 8, 2, mesh.shape["grp"]), ("shot_0", "shot_1", "shot_2", "grp")
    )
    return jax.shard_map(
        local,
        mesh=torus,
        in_specs=(P(SHOT_GRP, None, None), P(), P(SHOT_GRP, None), P(SHOT_GRP, None), P(SHOT_GRP)),
        out_specs=P(SHOT_GRP, None, None),
        check_vma=False,
    )
```

```python
import functools

import jax
import jax.numpy as jnp
from jax import lax
from jax.experimental import pallas as pl
from jax.experimental.pallas import tpu as pltpu
from jax.sharding import Mesh
from jax.sharding import PartitionSpec as P


SHOT_GRP = ("shot_0", "shot_1", "shot_2", "grp")
PLANE = ("shot_0", "shot_2", "grp")
RING = 8
LANES = 128
CAP = 2
PIECES = ((0, 5), (5, 8))


def pack_kernel(
    first, last, home_ref, tile_ref, slot_ref, live_ref, off_ref, *refs
):
    *total_ref, out_ref, data, zeros, flags, meta, meta_low, count = refs[:-3]
    in_sems, out_sem, meta_sem = refs[-3:]
    blocks, size, _ = off_ref.shape
    positions = flags.shape[0]
    quarters = data.shape[0]
    tiles = count.shape[0]
    slots = (last - first) * CAP
    parts = in_sems.shape[0]
    step = blocks // parts
    home = home_ref[0]

    def load(g, q):
        return pltpu.make_async_copy(
            off_ref.at[pl.ds(g * step, step), :, pl.ds(q * LANES, LANES)],
            data.at[q, pl.ds(g * step, step)],
            in_sems.at[g],
        )

    for g in range(parts):
        for q in range(quarters):
            load(g, q).start()
    zeros[...] = jnp.zeros_like(zeros)
    meta[...] = jnp.zeros_like(meta)

    def clear(t, _):
        count[t] = 0
        return 0

    lax.fori_loop(0, tiles, clear, 0)
    live = live_ref[...].astype(jnp.float32)
    twice = jnp.concatenate([live, live], axis=0)
    for low in range(0, positions, LANES):
        high = min(low + LANES, positions)
        turned = twice[:, low:high].T
        odd = lax.broadcasted_iota(jnp.int32, turned.shape, 0) % 2 == 1
        upper = lax.broadcasted_iota(jnp.int32, turned.shape, 1) >= LANES // 2
        flags[low:high, :] = jnp.where(odd == upper, turned, 0.0)

    def place(tile):
        ahead = ((tile // 2) % RING - home + RING) % RING
        near = jnp.minimum(ahead, RING - ahead)
        order = jnp.maximum(7 - 2 * near + (ahead > RING // 2).astype(jnp.int32), 0)
        column = (tile // (2 * RING)) * 2 + tile % 2
        mine = (order >= first) & (order < last)
        return column, (order - first) * CAP, mine

    def target(column, slot):
        return out_ref.at[column, :, pl.ds(pl.multiple_of(slot * size, size), size), :]

    def send(b, _):
        tile = tile_ref[b]
        rank = count[tile]
        count[tile] = rank + 1
        column, slot, mine = place(tile)

        @pl.when(mine)
        def _():
            pltpu.make_async_copy(data.at[:, b], target(column, slot + rank), out_sem).start()
            mark = (slot_ref[b] + 1).astype(jnp.float32)
            row = flags[pl.ds(2 * b, 1), :] + flags[pl.ds(2 * b + 1, 1), :]
            meta[column, pl.ds(slot + rank, 1), :] = row * mark

        return 0

    for g in range(parts):
        for q in range(quarters):
            load(g, q).wait()
        lax.fori_loop(g * step, (g + 1) * step, send, 0)

    def fill(tile, _):
        used = count[tile]
        column, slot, mine = place(tile)
        for rank in range(CAP):

            @pl.when(mine & (used <= rank))
            def _():
                pltpu.make_async_copy(zeros, target(column, slot + rank), out_sem).start()

        return 0

    lax.fori_loop(0, tiles, fill, 0)
    if total_ref:
        rest = total_ref[0][...]
        for term in range(3):
            part = rest.astype(jnp.bfloat16).astype(jnp.float32)
            rest = rest - part
            for column in range(meta.shape[0]):
                meta[column, slots + term : slots + term + 1, :] = part
    meta_low[...] = meta[...].astype(jnp.bfloat16)

    def meta_copy(q):
        return pltpu.make_async_copy(
            meta_low, out_ref.at[:, q, pl.ds(slots * size, meta.shape[1]), :], meta_sem
        )

    for q in range(quarters):
        meta_copy(q).start()
    whole = out_ref.at[:, :, pl.ds(0, slots * size), :]
    pltpu.make_async_copy(whole, whole, out_sem).wait()
    for q in range(quarters):
        meta_copy(q).wait()


def pack(piece, home, tiles, slots, live, blocks, carried, columns, quarters, tile_count):
    first, last = piece
    count, size, _ = blocks.shape
    rows = (last - first) * CAP
    meta_rows = -(-(rows + 3 * len(carried)) // 16) * 16
    vmem = pl.BlockSpec(memory_space=pltpu.VMEM)
    parts = 8
    hbm = pl.BlockSpec(memory_space=pltpu.HBM)
    smem = pl.BlockSpec(memory_space=pltpu.SMEM)
    return pl.pallas_call(
        functools.partial(pack_kernel, first, last),
        out_shape=jax.ShapeDtypeStruct(
            (columns, quarters, rows * size + meta_rows, LANES), jnp.bfloat16
        ),
        in_specs=[smem, smem, smem, vmem, hbm] + [vmem] * len(carried),
        out_specs=hbm,
        scratch_shapes=[
            pltpu.VMEM((quarters, count, size, LANES), jnp.bfloat16),
            pltpu.VMEM((quarters, size, LANES), jnp.bfloat16),
            pltpu.VMEM((2 * count, LANES), jnp.float32),
            pltpu.VMEM((columns, meta_rows, LANES), jnp.float32),
            pltpu.VMEM((columns, meta_rows, LANES), jnp.bfloat16),
            pltpu.SMEM((tile_count,), jnp.int32),
            pltpu.SemaphoreType.DMA((parts,)),
            pltpu.SemaphoreType.DMA,
            pltpu.SemaphoreType.DMA,
        ],
        compiler_params=pltpu.CompilerParams(vmem_limit_bytes=60 * 2**20),
        cost_estimate=pl.CostEstimate(
            flops=8_000_000_000, bytes_accessed=10 * 2**20, transcendentals=0
        ),
    )(home, tiles, slots, live, blocks, *carried)


def stack_kernel(slots, shift, code_ref, w_ref, in_ref, out_ref, acc):
    place, step = pl.program_id(0), pl.program_id(1)
    per, _, _ = in_ref.shape
    traces, lanes = acc.shape[1:]
    angles = traces // 2

    @pl.when(step == 0)
    def _():
        acc[...] = jnp.zeros_like(acc)

    row = lax.broadcasted_iota(jnp.int32, (angles, lanes), 0)
    for u in range(per):
        product = jnp.dot(w_ref[...], in_ref[u], preferred_element_type=jnp.float32)
        for j in range(CAP):
            code = code_ref[(step * per + u) * slots + (shift + place) * CAP + j]
            label = code >> 14
            for half, cut in enumerate(((code >> 7) & 127, code & 127)):
                low = half * angles
                angle = product[j * traces + low : j * traces + low + angles]
                angle = jnp.where(row < cut, angle, 0.0).astype(jnp.bfloat16)
                acc[label, low : low + angles, :] += angle.astype(jnp.float32)

    @pl.when(step == pl.num_programs(1) - 1)
    def _():
        out_ref[0] = acc[: out_ref.shape[1]].astype(out_ref.dtype)


def codes(arrived, slots, size, tile_rows):
    flags = arrived[:, slots * size : slots * size + slots, :].astype(jnp.int32)
    lane = lax.broadcasted_iota(jnp.int32, flags.shape, 2)
    live = (flags > 0).astype(jnp.int32) * jnp.where(lane < LANES // 2, 128, 1)
    label = jnp.where(flags > 0, flags - 1, tile_rows) * 16384
    return jnp.sum(live + jnp.where(lane == 0, label, 0), axis=2).reshape(-1)


def stack(code, weights, arrived, slots, shift, count, tile_rows, traces, dtype):
    sources, _, lanes = arrived.shape
    depth = weights.shape[1]
    per = 16
    return pl.pallas_call(
        functools.partial(stack_kernel, slots, shift),
        grid=(count, sources // per),
        out_shape=jax.ShapeDtypeStruct((count, tile_rows, traces, lanes), dtype),
        in_specs=[
            pl.BlockSpec(memory_space=pltpu.SMEM),
            pl.BlockSpec(weights.shape, lambda d, i: (0, 0)),
            pl.BlockSpec((per, depth, lanes), lambda d, i: (i, shift + d, 0)),
        ],
        out_specs=pl.BlockSpec((1, tile_rows, traces, lanes), lambda d, i: (d, 0, 0, 0)),
        scratch_shapes=[pltpu.VMEM((tile_rows + 1, traces, lanes), jnp.float32)],
        compiler_params=pltpu.CompilerParams(vmem_limit_bytes=16 * 2**20),
        cost_estimate=pl.CostEstimate(
            flops=2_500_000_000 * count, bytes_accessed=2**21 * count, transcendentals=0
        ),
    )(code, weights, arrived)


def join_kernel(half, rising_ref, falling_ref, own_ref, up_ref, down_ref):
    def added(out, passed, own, low, high):
        value = passed.astype(jnp.float32) + own_ref[own, low:high].astype(jnp.float32)
        out[low:high] = value.astype(out.dtype)

    rows = up_ref.shape[0]
    if half:
        middle = rows // 2
        added(up_ref, rising_ref[...], 0, 0, middle)
        up_ref[middle:] = own_ref[0, middle:]
        down_ref[:middle] = own_ref[1, :middle]
        added(down_ref, falling_ref[...], 1, middle, rows)
    else:
        added(up_ref, rising_ref[...], 0, 0, rows)
        added(down_ref, falling_ref[...], 1, 0, rows)


def join(half, rising, falling, own, pair):
    vmem = pl.BlockSpec(memory_space=pltpu.VMEM)
    shape = jax.ShapeDtypeStruct(own.shape[1:], own.dtype)
    block = (2,) + own.shape[1:]
    return pl.pallas_call(
        functools.partial(join_kernel, half),
        grid=(1,),
        out_shape=(shape, shape),
        in_specs=[vmem, vmem, pl.BlockSpec(block, lambda i: (pair, 0, 0, 0))],
        out_specs=(vmem, vmem),
        compiler_params=pltpu.CompilerParams(vmem_limit_bytes=16 * 2**20),
        cost_estimate=pl.CostEstimate(
            flops=1_000_000_000, bytes_accessed=3 * 2**20, transcendentals=0
        ),
        name="join",
    )(rising, falling, own)


def moments_kernel(group, cut_ref, w_ref, in_ref, out_ref):
    step = pl.program_id(0)
    angles, lanes = out_ref.shape
    count, hh, depth = in_ref.shape

    @pl.when(step == 0)
    def _():
        out_ref[...] = jnp.zeros_like(out_ref)

    row = lax.broadcasted_iota(jnp.int32, (angles, lanes), 0)
    total = out_ref[...]
    for part in range(count // group):
        gathers = in_ref[part * group : (part + 1) * group].reshape(group * hh, depth)
        square = None
        for q in range(depth // lanes):
            product = jnp.dot(
                w_ref[...],
                gathers[:, q * lanes : (q + 1) * lanes],
                preferred_element_type=jnp.float32,
            )
            product = product.astype(jnp.bfloat16).astype(jnp.float32)
            square = product * product if square is None else square + product * product
        for j in range(group):
            cut = cut_ref[step * count + part * group + j]
            total += jnp.where(row < cut, square[j * angles : (j + 1) * angles], 0.0)
    out_ref[...] = total


def moments(offsets, weights, live):
    positions, hh, depth = offsets.shape
    angles = live.shape[1]
    per = 16
    squares = pl.pallas_call(
        functools.partial(moments_kernel, weights.shape[0] // angles),
        grid=(positions // per,),
        out_shape=jax.ShapeDtypeStruct((angles, LANES), jnp.float32),
        in_specs=[
            pl.BlockSpec(memory_space=pltpu.SMEM),
            pl.BlockSpec(weights.shape, lambda i: (0, 0)),
            pl.BlockSpec((per, hh, depth), lambda i: (i, 0, 0)),
        ],
        out_specs=pl.BlockSpec((angles, LANES), lambda i: (0, 0)),
        compiler_params=pltpu.CompilerParams(vmem_limit_bytes=60 * 2**20),
        cost_estimate=pl.CostEstimate(
            flops=10_000_000_000, bytes_accessed=6 * 2**20, transcendentals=0
        ),
        name="moments",
    )(jnp.sum(live, axis=1), weights, offsets)
    return jnp.sum(squares, axis=1), jnp.sum(live, axis=0).astype(jnp.float32)


def finish_kernel(in_ref, out_ref):
    quarters, images, _, lanes = in_ref.shape
    for q in range(quarters):
        for k in range(images):
            out_ref[k, :, q * lanes : (q + 1) * lanes] = in_ref[q, k]


def finish(swapped):
    quarters, images, traces, lanes = swapped.shape
    vmem = pl.BlockSpec(memory_space=pltpu.VMEM)
    return pl.pallas_call(
        finish_kernel,
        out_shape=jax.ShapeDtypeStruct((images, traces, quarters * lanes), swapped.dtype),
        in_specs=[vmem],
        out_specs=vmem,
        name="finish",
    )(swapped)


def work(offsets, slant_weights, live, block_tile, image_slot):
    block_count = block_tile.shape[0]
    _, hh, depth = offsets.shape
    angles = slant_weights.shape[0]
    traces = 2 * angles
    size = 2 * hh
    tile_count = lax.axis_size(("shot_0", "shot_1", "shot_2"))
    columns = lax.axis_size(("shot_0", "shot_2"))
    quarters = lax.axis_size("grp")
    tile_rows = 4 * quarters
    blocks = offsets.reshape(block_count, size, depth)
    tiles = block_tile[:, 0]
    home = lax.axis_index("shot_1").reshape(1)
    up = [(i, (i + 1) % RING) for i in range(RING)]
    down = [(i, (i - 1) % RING) for i in range(RING)]

    def diagonal(count):
        return jnp.kron(jnp.eye(count, dtype=jnp.bfloat16), slant_weights)

    squares, counts = moments(offsets, diagonal(8), live)
    totals = jnp.concatenate([squares, counts])
    totals = lax.psum(totals, "shot_1")[None, :]

    pair = diagonal(2 * CAP)
    arrived, code = [], []
    for n, piece in enumerate(PIECES):
        slots = (piece[1] - piece[0]) * CAP
        carried = [totals] if n else []
        sent = pack(
            piece, home, tiles, image_slot, live.T, blocks, carried,
            columns, quarters, tile_count,
        )
        sent = sent.reshape((columns * quarters,) + sent.shape[2:])
        arrived.append(lax.all_to_all(sent, PLANE, 0, 0, tiled=True))
        code.append(codes(arrived[-1], slots, size, tile_rows))
    low = slots * (size + 1)
    totals = jnp.sum(arrived[1][:, low : low + 3].astype(jnp.float32), axis=(0, 1))
    gain = lax.rsqrt(totals[:angles] / (depth * totals[angles:]) + 1e-06)

    def stacked(n, shift, count, dtype):
        slots = (PIECES[n][1] - PIECES[n][0]) * CAP
        return stack(
            code[n], pair, arrived[n], slots, shift, count, tile_rows, traces, dtype
        )

    far = stacked(0, 0, 1, jnp.bfloat16)[0]
    rising = lax.ppermute(far[: tile_rows // 2], "shot_1", up)
    falling = lax.ppermute(far[tile_rows // 2 :], "shot_1", down)
    middle = stacked(0, 1, 4, jnp.bfloat16)
    near = stacked(1, 0, 2, jnp.bfloat16)
    for n, (parts, at) in enumerate(((middle, 0), (middle, 1), (near, 0))):
        rising, falling = join(n == 0, rising, falling, parts, at)
        rising = lax.ppermute(rising, "shot_1", up)
        falling = lax.ppermute(falling, "shot_1", down)
    own = stacked(1, 2, 1, jnp.float32)[0]
    total = own + rising.astype(jnp.float32) + falling.astype(jnp.float32)
    image = (total * jnp.tile(gain, 2)[None, :, None]).astype(jnp.bfloat16)
    image = image.reshape(quarters, 4, traces, LANES)
    swapped = lax.all_to_all(image, "grp", 0, 0, tiled=True)
    return finish(swapped)


def solution(mesh):
    torus = Mesh(
        mesh.devices.reshape(4, RING, 2, mesh.shape["grp"]),
        ("shot_0", "shot_1", "shot_2", "grp"),
    )
    return jax.shard_map(
        work,
        mesh=torus,
        in_specs=(P(SHOT_GRP, None, None), P(), P(SHOT_GRP, None), P(SHOT_GRP, None), P(SHOT_GRP)),
        out_specs=P(SHOT_GRP, None, None),
        check_vma=False,
    )
```

```python
import functools

import jax
import jax.numpy as jnp
from jax import lax
from jax.experimental import pallas as pl
from jax.experimental.pallas import tpu as pltpu
from jax.sharding import Mesh
from jax.sharding import PartitionSpec as P


SHOT_GRP = ("shot_0", "shot_1", "shot_2", "grp")
PLANE = ("shot_0", "shot_2", "grp")
RING = 8
LANES = 128
CAP = 2
PIECES = ((0, 5), (5, 8))


def pack_kernel(
    first, last, home_ref, tile_ref, slot_ref, live_ref, off_ref, *refs
):
    *total_ref, out_ref, data, zeros, flags, meta, meta_low, count, goal = refs[:-3]
    in_sems, out_sem, meta_sem = refs[-3:]
    blocks, size, _ = off_ref.shape
    positions = flags.shape[0]
    quarters = data.shape[0]
    tiles = count.shape[0]
    slots = (last - first) * CAP
    parts = in_sems.shape[0]
    step = blocks // parts
    home = home_ref[0]

    def load(g, q):
        return pltpu.make_async_copy(
            off_ref.at[pl.ds(g * step, step), :, pl.ds(q * LANES, LANES)],
            data.at[q, pl.ds(g * step, step)],
            in_sems.at[g],
        )

    for g in range(parts):
        for q in range(quarters):
            load(g, q).start()
    zeros[...] = jnp.zeros_like(zeros)
    meta[...] = jnp.zeros_like(meta)

    def clear(t, _):
        count[t] = 0
        return 0

    lax.fori_loop(0, tiles, clear, 0, unroll=8)
    live = live_ref[...].astype(jnp.float32)
    twice = jnp.concatenate([live, live], axis=0)
    for low in range(0, positions, LANES):
        high = min(low + LANES, positions)
        turned = twice[:, low:high].T
        odd = lax.broadcasted_iota(jnp.int32, turned.shape, 0) % 2 == 1
        upper = lax.broadcasted_iota(jnp.int32, turned.shape, 1) >= LANES // 2
        flags[low:high, :] = jnp.where(odd == upper, turned, 0.0)

    def place(tile):
        ahead = ((tile // 2) % RING - home + RING) % RING
        near = jnp.minimum(ahead, RING - ahead)
        order = jnp.maximum(7 - 2 * near + (ahead > RING // 2).astype(jnp.int32), 0)
        column = (tile // (2 * RING)) * 2 + tile % 2
        mine = (order >= first) & (order < last)
        return column, (order - first) * CAP, mine

    def target(column, slot):
        return out_ref.at[column, :, pl.ds(pl.multiple_of(slot * size, size), size), :]

    def plan(b, _):
        tile = tile_ref[b]
        rank = count[tile]
        count[tile] = rank + 1
        column, slot, mine = place(tile)
        goal[b] = jnp.where(mine, column * slots + slot + rank, -1)

        @pl.when(mine)
        def _():
            mark = (slot_ref[b] + 1).astype(jnp.float32)
            row = flags[pl.ds(2 * b, 1), :] + flags[pl.ds(2 * b + 1, 1), :]
            meta[column, pl.ds(slot + rank, 1), :] = row * mark

        return 0

    lax.fori_loop(0, blocks, plan, 0, unroll=4)

    def fill(tile, _):
        used = count[tile]
        column, slot, mine = place(tile)
        for rank in range(CAP):

            @pl.when(mine & (used <= rank))
            def _():
                pltpu.make_async_copy(zeros, target(column, slot + rank), out_sem).start()

        return 0

    lax.fori_loop(0, tiles, fill, 0, unroll=4)
    if total_ref:
        rest = total_ref[0][...]
        for term in range(3):
            part = rest.astype(jnp.bfloat16).astype(jnp.float32)
            rest = rest - part
            for column in range(meta.shape[0]):
                meta[column, slots + term : slots + term + 1, :] = part
    meta_low[...] = meta[...].astype(jnp.bfloat16)

    def send(b, _):
        at = goal[b]

        @pl.when(at >= 0)
        def _():
            pltpu.make_async_copy(
                data.at[:, b], target(at // slots, at % slots), out_sem
            ).start()

        return 0

    def meta_copy(q):
        return pltpu.make_async_copy(
            meta_low, out_ref.at[:, q, pl.ds(slots * size, meta.shape[1]), :], meta_sem
        )

    for g in range(parts):
        for q in range(quarters):
            load(g, q).wait()
        lax.fori_loop(g * step, (g + 1) * step, send, 0, unroll=4)
        if g == parts // 2:
            for q in range(quarters):
                meta_copy(q).start()
    whole = out_ref.at[:, :, pl.ds(0, slots * size), :]
    pltpu.make_async_copy(whole, whole, out_sem).wait()
    for q in range(quarters):
        meta_copy(q).wait()


def pack(piece, home, tiles, slots, live, blocks, carried, columns, quarters, tile_count):
    first, last = piece
    count, size, _ = blocks.shape
    rows = (last - first) * CAP
    meta_rows = -(-(rows + 3 * len(carried)) // 16) * 16
    vmem = pl.BlockSpec(memory_space=pltpu.VMEM)
    parts = 8
    hbm = pl.BlockSpec(memory_space=pltpu.HBM)
    smem = pl.BlockSpec(memory_space=pltpu.SMEM)
    return pl.pallas_call(
        functools.partial(pack_kernel, first, last),
        out_shape=jax.ShapeDtypeStruct(
            (columns, quarters, rows * size + meta_rows, LANES), jnp.bfloat16
        ),
        in_specs=[smem, smem, smem, vmem, hbm] + [vmem] * len(carried),
        out_specs=hbm,
        scratch_shapes=[
            pltpu.VMEM((quarters, count, size, LANES), jnp.bfloat16),
            pltpu.VMEM((quarters, size, LANES), jnp.bfloat16),
            pltpu.VMEM((2 * count, LANES), jnp.float32),
            pltpu.VMEM((columns, meta_rows, LANES), jnp.float32),
            pltpu.VMEM((columns, meta_rows, LANES), jnp.bfloat16),
            pltpu.SMEM((tile_count,), jnp.int32),
            pltpu.SMEM((count,), jnp.int32),
            pltpu.SemaphoreType.DMA((parts,)),
            pltpu.SemaphoreType.DMA,
            pltpu.SemaphoreType.DMA,
        ],
        compiler_params=pltpu.CompilerParams(vmem_limit_bytes=60 * 2**20),
        cost_estimate=pl.CostEstimate(
            flops=8_000_000_000, bytes_accessed=10 * 2**20, transcendentals=0
        ),
    )(home, tiles, slots, live, blocks, *carried)


def stack_kernel(slots, shift, joined, code_ref, w_ref, in_ref, *refs):
    acc = refs[-1]
    place, step = pl.program_id(0), pl.program_id(1)
    per, _, _ = in_ref.shape
    traces, lanes = acc.shape[1:]
    angles = traces // 2

    if joined:
        passed = (refs[0:2], refs[2:4])
        images = passed[0][0].shape[0]
        for at in range(2):

            @pl.when((step == 0) & (place == at))
            def _():
                for half in range(2):
                    acc[:images, half * angles : (half + 1) * angles] = passed[at][half][
                        ...
                    ].astype(jnp.float32)
    else:

        @pl.when(step == 0)
        def _():
            acc[...] = jnp.zeros_like(acc)

    row = lax.broadcasted_iota(jnp.int32, (angles, lanes), 0)
    for u in range(per):
        product = jnp.dot(w_ref[...], in_ref[u], preferred_element_type=jnp.float32)
        for j in range(CAP):
            code = code_ref[(step * per + u) * slots + (shift + place) * CAP + j]
            label = code >> 14
            for half, cut in enumerate(((code >> 7) & 127, code & 127)):
                low = half * angles
                angle = product[j * traces + low : j * traces + low + angles]
                angle = jnp.where(row < cut, angle, 0.0).astype(jnp.bfloat16)
                acc[label, low : low + angles, :] += angle.astype(jnp.float32)

    outs = (refs[4:6], refs[6:8]) if joined else (refs[0:2],)
    for at, pair in enumerate(outs):

        @pl.when((step == pl.num_programs(1) - 1) & ((place == at) | (not joined)))
        def _():
            for half, ref in enumerate(pair):
                images = ref.shape[-3]
                value = acc[:images, half * angles : (half + 1) * angles]
                ref[...] = value.astype(ref.dtype).reshape(ref.shape)


def codes(arrived, slots, size, tile_rows):
    flags = arrived[:, slots * size : slots * size + slots, :].astype(jnp.int32)
    lane = lax.broadcasted_iota(jnp.int32, flags.shape, 2)
    live = (flags > 0).astype(jnp.int32) * jnp.where(lane < LANES // 2, 128, 1)
    label = jnp.where(flags > 0, flags - 1, tile_rows) * 16384
    return jnp.sum(live + jnp.where(lane == 0, label, 0), axis=2).reshape(-1)


def stack(code, weights, arrived, slots, shift, count, tile_rows, traces, dtype, passed=()):
    sources, _, lanes = arrived.shape
    depth = weights.shape[1]
    per = 16
    half = (tile_rows, traces // 2, lanes)
    shape = jax.ShapeDtypeStruct((count,) + half, dtype)
    spec = pl.BlockSpec((1,) + half, lambda d, i: (d, 0, 0, 0))
    outs, specs = (shape, shape), (spec, spec)
    if passed:
        outs = (jax.ShapeDtypeStruct(half, dtype),) * 4
        specs = (pl.BlockSpec(memory_space=pltpu.VMEM),) * 4
    return pl.pallas_call(
        functools.partial(stack_kernel, slots, shift, bool(passed)),
        grid=(count, sources // per),
        out_shape=outs,
        in_specs=[
            pl.BlockSpec(memory_space=pltpu.SMEM),
            pl.BlockSpec(weights.shape, lambda d, i: (0, 0)),
            pl.BlockSpec((per, depth, lanes), lambda d, i: (i, shift + d, 0)),
        ]
        + [pl.BlockSpec(memory_space=pltpu.VMEM)] * len(passed),
        out_specs=specs,
        scratch_shapes=[pltpu.VMEM((tile_rows + 1, traces, lanes), jnp.float32)],
        compiler_params=pltpu.CompilerParams(vmem_limit_bytes=16 * 2**20),
        cost_estimate=pl.CostEstimate(
            flops=2_500_000_000 * count, bytes_accessed=2**21 * count, transcendentals=0
        ),
    )(code, weights, arrived, *passed)


def join_kernel(at, passed_ref, own_ref, out_ref):
    value = passed_ref[...].astype(jnp.float32) + own_ref[at].astype(jnp.float32)
    out_ref[...] = value.astype(out_ref.dtype)


def join(passed, own, at):
    vmem = pl.BlockSpec(memory_space=pltpu.VMEM)
    return pl.pallas_call(
        functools.partial(join_kernel, at),
        out_shape=jax.ShapeDtypeStruct(passed.shape, passed.dtype),
        in_specs=[vmem, vmem],
        out_specs=vmem,
        compiler_params=pltpu.CompilerParams(vmem_limit_bytes=8 * 2**20),
        cost_estimate=pl.CostEstimate(
            flops=500_000_000, bytes_accessed=2**20, transcendentals=0
        ),
        name="join",
    )(passed, own)


def total_kernel(side_ref, gain_ref, own_ref, rising_ref, falling_ref, *out_refs):
    images = out_refs[0].shape[0]
    gain = gain_ref[...]
    for k, out_ref in enumerate(out_refs):
        start = (side_ref[0] + k) % len(out_refs) * images
        for i in range(images):
            value = own_ref[0, start + i] + rising_ref[start + i].astype(jnp.float32)
            value = (value + falling_ref[start + i].astype(jnp.float32)) * gain
            out_ref[i] = value.astype(out_ref.dtype)


def total(side, gain, own, rising, falling, quarters):
    vmem = pl.BlockSpec(memory_space=pltpu.VMEM)
    rows, angles, lanes = rising.shape
    shape = jax.ShapeDtypeStruct((rows // quarters, angles, lanes), jnp.bfloat16)
    return pl.pallas_call(
        total_kernel,
        out_shape=(shape,) * quarters,
        in_specs=[pl.BlockSpec(memory_space=pltpu.SMEM), vmem, vmem, vmem, vmem],
        out_specs=(vmem,) * quarters,
        compiler_params=pltpu.CompilerParams(vmem_limit_bytes=8 * 2**20),
        cost_estimate=pl.CostEstimate(
            flops=500_000_000, bytes_accessed=2**20, transcendentals=0
        ),
        name="total",
    )(side, gain, own, rising, falling)


def moments_kernel(group, cut_ref, w_ref, in_ref, out_ref):
    step = pl.program_id(0)
    angles, lanes = out_ref.shape
    count, hh, depth = in_ref.shape

    @pl.when(step == 0)
    def _():
        out_ref[...] = jnp.zeros_like(out_ref)

    row = lax.broadcasted_iota(jnp.int32, (angles, lanes), 0)
    total = out_ref[...]
    for part in range(count // group):
        gathers = in_ref[part * group : (part + 1) * group].reshape(group * hh, depth)
        square = None
        for q in range(depth // lanes):
            product = jnp.dot(
                w_ref[...],
                gathers[:, q * lanes : (q + 1) * lanes],
                preferred_element_type=jnp.float32,
            )
            product = product.astype(jnp.bfloat16).astype(jnp.float32)
            square = product * product if square is None else square + product * product
        for j in range(group):
            cut = cut_ref[step * count + part * group + j]
            total += jnp.where(row < cut, square[j * angles : (j + 1) * angles], 0.0)
    out_ref[...] = total


def moments(offsets, weights, live):
    positions, hh, depth = offsets.shape
    angles = live.shape[1]
    per = 16
    squares = pl.pallas_call(
        functools.partial(moments_kernel, weights.shape[0] // angles),
        grid=(positions // per,),
        out_shape=jax.ShapeDtypeStruct((angles, LANES), jnp.float32),
        in_specs=[
            pl.BlockSpec(memory_space=pltpu.SMEM),
            pl.BlockSpec(weights.shape, lambda i: (0, 0)),
            pl.BlockSpec((per, hh, depth), lambda i: (i, 0, 0)),
        ],
        out_specs=pl.BlockSpec((angles, LANES), lambda i: (0, 0)),
        compiler_params=pltpu.CompilerParams(vmem_limit_bytes=60 * 2**20),
        cost_estimate=pl.CostEstimate(
            flops=10_000_000_000, bytes_accessed=6 * 2**20, transcendentals=0
        ),
        name="moments",
    )(jnp.sum(live, axis=1), weights, offsets)
    return jnp.sum(squares, axis=1), jnp.sum(live, axis=0).astype(jnp.float32)


def finish_kernel(side_ref, *refs):
    out_ref = refs[-1]
    halves = (refs[: len(refs) // 2], refs[len(refs) // 2 : -1])
    angles, lanes = refs[0].shape[1:]
    for half, parts in enumerate(halves):
        for k, ref in enumerate(parts):
            quarter = (side_ref[0] - k + len(parts)) % len(parts)
            start = pl.multiple_of(quarter * lanes, lanes)
            out_ref[:, half * angles : (half + 1) * angles, pl.ds(start, lanes)] = ref[...]


def finish(side, first, second):
    images, angles, lanes = first[0].shape
    vmem = pl.BlockSpec(memory_space=pltpu.VMEM)
    return pl.pallas_call(
        finish_kernel,
        out_shape=jax.ShapeDtypeStruct((images, 2 * angles, len(first) * lanes), jnp.bfloat16),
        in_specs=[pl.BlockSpec(memory_space=pltpu.SMEM)] + [vmem] * (2 * len(first)),
        out_specs=vmem,
        compiler_params=pltpu.CompilerParams(vmem_limit_bytes=8 * 2**20),
        name="finish",
    )(side, *first, *second)


def work(offsets, slant_weights, live, block_tile, image_slot):
    block_count = block_tile.shape[0]
    _, hh, depth = offsets.shape
    angles = slant_weights.shape[0]
    traces = 2 * angles
    size = 2 * hh
    tile_count = lax.axis_size(("shot_0", "shot_1", "shot_2"))
    columns = lax.axis_size(("shot_0", "shot_2"))
    quarters = lax.axis_size("grp")
    tile_rows = 4 * quarters
    blocks = offsets.reshape(block_count, size, depth)
    tiles = block_tile[:, 0]
    home = lax.axis_index("shot_1").reshape(1)

    def diagonal(count):
        return jnp.kron(jnp.eye(count, dtype=jnp.bfloat16), slant_weights)

    squares, counts = moments(offsets, diagonal(8), live)
    totals = jnp.concatenate([squares, counts])
    totals = lax.psum(totals, "shot_1")[None, :]

    pair = diagonal(2 * CAP)
    arrived, code = [], []
    for n, piece in enumerate(PIECES):
        slots = (piece[1] - piece[0]) * CAP
        carried = [totals] if n == 1 else []
        sent = pack(
            piece, home, tiles, image_slot, live.T, blocks, carried,
            columns, quarters, tile_count,
        )
        if n == 1:
            low = slots * (size + 1)
        sent = sent.reshape((columns * quarters,) + sent.shape[2:])
        arrived.append(lax.all_to_all(sent, PLANE, 0, 0, tiled=True))
        code.append(codes(arrived[-1], slots, size, tile_rows))
    totals = jnp.sum(arrived[1][:, low : low + 3].astype(jnp.float32), axis=(0, 1))
    gain = lax.rsqrt(totals[:angles] / (depth * totals[angles:]) + 1e-06)

    def stacked(n, shift, count, dtype, passed=()):
        slots = (PIECES[n][1] - PIECES[n][0]) * CAP
        return stack(
            code[n], pair, arrived[n], slots, shift, count, tile_rows, traces, dtype, passed
        )

    def move(array, axis, shift):
        count = lax.axis_size(axis)
        return lax.ppermute(array, axis, [(i, (i + shift) % count) for i in range(count)])

    far = stacked(0, 0, 1, jnp.bfloat16)
    rising = [move(far[0][0], "shot_1", 1), None]
    falling = [None, move(far[1][0], "shot_1", -1)]
    for place in ((0, 1), (0, 3)):
        parts = stacked(*place, 2, jnp.bfloat16)
        for half in range(2):
            for chain, at, shift in ((rising, 0, 1), (falling, 1, -1)):
                if chain[half] is None:
                    chain[half] = parts[half][at]
                else:
                    chain[half] = join(chain[half], parts[half], at)
                chain[half] = move(chain[half], "shot_1", shift)
    parts = stacked(1, 0, 2, jnp.bfloat16, rising + falling)
    for half in (1, 0):
        rising[half] = move(parts[half], "shot_1", 1)
        falling[half] = move(parts[2 + half], "shot_1", -1)
    own = stacked(1, 2, 1, jnp.float32)
    side = lax.axis_index("grp").reshape(1)
    scale = jnp.broadcast_to(gain[:, None], (angles, LANES))
    ends = []
    for half in range(2):
        parts = total(side, scale, own[half], rising[half], falling[half], quarters)
        ends.append([parts[0]] + [move(parts[k], "grp", k) for k in range(1, quarters)])
    return finish(side, *ends)


def solution(mesh):
    torus = Mesh(
        mesh.devices.reshape(4, RING, 2, mesh.shape["grp"]),
        ("shot_0", "shot_1", "shot_2", "grp"),
    )
    return jax.shard_map(
        work,
        mesh=torus,
        in_specs=(P(SHOT_GRP, None, None), P(), P(SHOT_GRP, None), P(SHOT_GRP, None), P(SHOT_GRP)),
        out_specs=P(SHOT_GRP, None, None),
        check_vma=False,
    )
```

```python
import functools

import jax
import jax.numpy as jnp
from jax import lax
from jax.experimental import pallas as pl
from jax.experimental.pallas import tpu as pltpu
from jax.sharding import Mesh
from jax.sharding import PartitionSpec as P


SHOT_GRP = ("shot_0", "shot_1", "shot_2", "grp")
PLANE = ("shot_0", "shot_2", "grp")
RING = 8
LANES = 128
CAP = 2
FAR = (0, 5)


def pack_kernel(
    first, last, groups, carry, moved, home_ref, tile_ref, slot_ref, live_ref, off_ref, *refs
):
    total_ref, moved_refs = refs[:carry], refs[carry : carry + moved]
    out_refs = refs[carry + moved : carry + moved + groups]
    data, zeros, flags, meta, meta_low, count, goal = refs[carry + moved + groups :][:7]
    in_sems, out_sem, meta_sem, moved_sem = refs[-4:]
    blocks, size, _ = off_ref.shape
    positions = flags.shape[0]
    quarters = data.shape[0]
    tiles = count.shape[0]
    slots = (last - first) // groups * CAP
    columns = out_refs[0].shape[0]
    meta_at = slots * size * (1 + moved)
    meta_rows = meta.shape[1]
    parts = in_sems.shape[0]
    step = blocks // parts
    home = home_ref[0]

    def load(g, q):
        return pltpu.make_async_copy(
            off_ref.at[pl.ds(g * step, step), :, pl.ds(q * LANES, LANES)],
            data.at[q, pl.ds(g * step, step)],
            in_sems.at[g],
        )

    for g in range(parts):
        for q in range(quarters):
            load(g, q).start()

    def pass_on(m):
        rows = slots * size
        moves = (
            (0, (m + 1) * rows, rows),
            (rows, meta_at + (m + 1) * meta_rows, meta_rows),
        )
        return [
            pltpu.make_async_copy(
                moved_refs[m].at[:, :, pl.ds(source, length), :],
                out_refs[0].at[:, :, pl.ds(goal_row, length), :],
                moved_sem.at[2 * m + n],
            )
            for n, (source, goal_row, length) in enumerate(moves)
        ]

    for m in range(moved):
        for copy in pass_on(m):
            copy.start()
    zeros[...] = jnp.zeros_like(zeros)
    meta[...] = jnp.zeros_like(meta)

    def clear(t, _):
        count[t] = 0
        return 0

    lax.fori_loop(0, tiles, clear, 0, unroll=8)
    live = live_ref[...].astype(jnp.float32)
    twice = jnp.concatenate([live, live], axis=0)
    for low in range(0, positions, LANES):
        high = min(low + LANES, positions)
        turned = twice[:, low:high].T
        odd = lax.broadcasted_iota(jnp.int32, turned.shape, 0) % 2 == 1
        upper = lax.broadcasted_iota(jnp.int32, turned.shape, 1) >= LANES // 2
        flags[low:high, :] = jnp.where(odd == upper, turned, 0.0)

    def place(tile):
        ahead = ((tile // 2) % RING - home + RING) % RING
        near = jnp.minimum(ahead, RING - ahead)
        order = jnp.maximum(7 - 2 * near + (ahead > RING // 2).astype(jnp.int32), 0)
        column = (tile // (2 * RING)) * 2 + tile % 2
        mine = (order >= first) & (order < last)
        if groups > 1:
            return (order - first) * columns + column, 0, mine
        return column, (order - first) * CAP, mine

    def start(source, line, slot):
        rows = pl.ds(pl.multiple_of(slot * size, size), size)
        for k, out_ref in enumerate(out_refs):
            if groups == 1:
                target = out_ref.at[line, :, rows, :]
                pltpu.make_async_copy(source, target, out_sem).start()
            else:

                @pl.when((line >= k * columns) & (line < (k + 1) * columns))
                def _():
                    target = out_ref.at[line - k * columns, :, rows, :]
                    pltpu.make_async_copy(source, target, out_sem).start()

    def plan(b, _):
        tile = tile_ref[b]
        rank = count[tile]
        count[tile] = rank + 1
        column, slot, mine = place(tile)
        goal[b] = jnp.where(mine, column * 64 + slot + rank, -1)

        @pl.when(mine)
        def _():
            mark = (slot_ref[b] + 1).astype(jnp.float32)
            row = flags[pl.ds(2 * b, 1), :] + flags[pl.ds(2 * b + 1, 1), :]
            meta[column, pl.ds(slot + rank, 1), :] = row * mark

        return 0

    lax.fori_loop(0, blocks, plan, 0, unroll=4)

    def fill(tile, _):
        used = count[tile]
        column, slot, mine = place(tile)
        for rank in range(CAP):

            @pl.when(mine & (used <= rank))
            def _():
                start(zeros, column, slot + rank)

        return 0

    lax.fori_loop(0, tiles, fill, 0, unroll=4)
    if total_ref:
        rest = total_ref[0][...]
        for term in range(3):
            part = rest.astype(jnp.bfloat16).astype(jnp.float32)
            rest = rest - part
            for column in range(meta.shape[0]):
                meta[column, slots + term : slots + term + 1, :] = part
    meta_low[...] = meta[...].astype(jnp.bfloat16)

    def send(b, _):
        at = goal[b]

        @pl.when(at >= 0)
        def _():
            start(data.at[:, b], at >> 6, at & 63)

        return 0

    def meta_copies():
        return [
            pltpu.make_async_copy(
                meta_low.at[pl.ds(k * columns, columns)],
                out_ref.at[:, q, pl.ds(meta_at, meta_rows), :],
                meta_sem,
            )
            for k, out_ref in enumerate(out_refs)
            for q in range(quarters)
        ]

    for g in range(parts):
        for q in range(quarters):
            load(g, q).wait()
        lax.fori_loop(g * step, (g + 1) * step, send, 0, unroll=4)
        if g == parts // 2:
            for copy in meta_copies():
                copy.start()
    for out_ref in out_refs:
        whole = out_ref.at[:, :, pl.ds(0, slots * size), :]
        pltpu.make_async_copy(whole, whole, out_sem).wait()
    for copy in meta_copies():
        copy.wait()
    for m in range(moved):
        for copy in pass_on(m):
            copy.wait()


def pack(
    piece, home, tiles, slots, live, blocks, columns, quarters, tile_count,
    groups=1, carried=(), moved=(),
):
    first, last = piece
    count, size, _ = blocks.shape
    rows = (last - first) // groups * CAP
    meta_rows = -(-(rows + 3 * len(carried)) // 8) * 8
    length = (rows * size + meta_rows) * (1 + len(moved))
    parts = 8
    vmem = pl.BlockSpec(memory_space=pltpu.VMEM)
    hbm = pl.BlockSpec(memory_space=pltpu.HBM)
    smem = pl.BlockSpec(memory_space=pltpu.SMEM)
    shape = jax.ShapeDtypeStruct((columns, quarters, length, LANES), jnp.bfloat16)
    return pl.pallas_call(
        functools.partial(pack_kernel, first, last, groups, len(carried), len(moved)),
        out_shape=(shape,) * groups,
        in_specs=[smem, smem, smem, vmem, hbm] + [vmem] * (len(carried) + len(moved)),
        out_specs=(hbm,) * groups,
        scratch_shapes=[
            pltpu.VMEM((quarters, count, size, LANES), jnp.bfloat16),
            pltpu.VMEM((quarters, size, LANES), jnp.bfloat16),
            pltpu.VMEM((2 * count, LANES), jnp.float32),
            pltpu.VMEM((groups * columns, meta_rows, LANES), jnp.float32),
            pltpu.VMEM((groups * columns, meta_rows, LANES), jnp.bfloat16),
            pltpu.SMEM((tile_count,), jnp.int32),
            pltpu.SMEM((count,), jnp.int32),
            pltpu.SemaphoreType.DMA((parts,)),
            pltpu.SemaphoreType.DMA,
            pltpu.SemaphoreType.DMA,
            pltpu.SemaphoreType.DMA((max(2 * len(moved), 1),)),
        ],
        compiler_params=pltpu.CompilerParams(
            vmem_limit_bytes=62 * 2**20
        ),
        cost_estimate=pl.CostEstimate(
            flops=8_000_000_000, bytes_accessed=10 * 2**20, transcendentals=0
        ),
    )(home, tiles, slots, live, blocks, *carried, *moved)


def stack_kernel(codes_each, stride, shift, merge, code_ref, w_ref, in_ref, first_ref, second_ref, acc):
    place, step = pl.program_id(0), pl.program_id(1)
    per = in_ref.shape[0]
    traces, lanes = acc.shape[1:]
    angles = traces // 2
    begins, ends = step == 0, step == pl.num_programs(1) - 1
    if merge:
        begins = begins & (place == 0)
        ends = ends & (place == pl.num_programs(0) - 1)

    @pl.when(begins)
    def _():
        acc[...] = jnp.zeros_like(acc)

    weights = w_ref[...].T
    row = lax.broadcasted_iota(jnp.int32, (angles, lanes), 0)
    for u in range(per):
        product = jnp.dot(weights, in_ref[u], preferred_element_type=jnp.float32)
        for j in range(CAP):
            code = code_ref[(step * per + u) * codes_each + (shift + place) * stride + j]
            label = code >> 14
            for half, cut in enumerate(((code >> 7) & 127, code & 127)):
                low = half * angles
                angle = product[j * traces + low : j * traces + low + angles]
                angle = jnp.where(row < cut, angle, 0.0).astype(jnp.bfloat16)
                acc[label, low : low + angles, :] += angle.astype(jnp.float32)

    @pl.when(ends)
    def _():
        images = first_ref.shape[1]
        first_ref[0] = acc[:images, :angles].astype(first_ref.dtype)
        second_ref[0] = acc[:images, angles:].astype(second_ref.dtype)


def codes(arrived, rows, tile_rows):
    flags = arrived[:, rows:].astype(jnp.int32)
    lane = lax.broadcasted_iota(jnp.int32, flags.shape, 2)
    live = (flags > 0).astype(jnp.int32) * jnp.where(lane < LANES // 2, 128, 1)
    label = jnp.where(flags > 0, flags - 1, tile_rows) * 16384
    return jnp.sum(live + jnp.where(lane == 0, label, 0), axis=2).reshape(-1)


def stack(code, weights, arrived, shift, count, stride, merge, tile_rows, traces, dtype):
    sources, _, lanes = arrived.shape
    codes_each = code.shape[0] // sources
    height = weights.shape[0]
    per = 16
    half = (tile_rows, traces // 2, lanes)
    shape = jax.ShapeDtypeStruct((1 if merge else count,) + half, dtype)
    spec = pl.BlockSpec((1,) + half, lambda d, i: (0 if merge else d, 0, 0, 0))
    return pl.pallas_call(
        functools.partial(stack_kernel, codes_each, stride, shift, merge),
        grid=(count, sources // per),
        out_shape=(shape, shape),
        in_specs=[
            pl.BlockSpec(memory_space=pltpu.SMEM),
            pl.BlockSpec(weights.shape, lambda d, i: (0, 0)),
            pl.BlockSpec((per, height, lanes), lambda d, i: (i, shift + d, 0)),
        ],
        out_specs=(spec, spec),
        scratch_shapes=[pltpu.VMEM((tile_rows + 1, traces, lanes), jnp.float32)],
        compiler_params=pltpu.CompilerParams(
            vmem_limit_bytes=(44 if merge else 16) * 2**20
        ),
        cost_estimate=pl.CostEstimate(
            flops=2_500_000_000 * count, bytes_accessed=2**21 * count, transcendentals=0
        ),
    )(code, weights, arrived)


def join_kernel(at, passed_ref, own_ref, out_ref):
    value = passed_ref[...].astype(jnp.float32) + own_ref[at].astype(jnp.float32)
    out_ref[...] = value.astype(out_ref.dtype)


def join(passed, own, at):
    vmem = pl.BlockSpec(memory_space=pltpu.VMEM)
    return pl.pallas_call(
        functools.partial(join_kernel, at),
        out_shape=jax.ShapeDtypeStruct(passed.shape, passed.dtype),
        in_specs=[vmem, vmem],
        out_specs=vmem,
        compiler_params=pltpu.CompilerParams(vmem_limit_bytes=8 * 2**20),
        cost_estimate=pl.CostEstimate(
            flops=500_000_000, bytes_accessed=2**20, transcendentals=0
        ),
        name="join",
    )(passed, own)


def total_kernel(side_ref, gain_ref, own_ref, rising_ref, falling_ref, *out_refs):
    images = out_refs[0].shape[0]
    gain = gain_ref[...]
    for k, out_ref in enumerate(out_refs):
        start = (side_ref[0] + k) % len(out_refs) * images
        for i in range(images):
            value = own_ref[0, start + i].astype(jnp.float32) + rising_ref[start + i].astype(jnp.float32)
            value = (value + falling_ref[start + i].astype(jnp.float32)) * gain
            out_ref[i] = value.astype(out_ref.dtype)


def total(side, gain, own, rising, falling, quarters):
    vmem = pl.BlockSpec(memory_space=pltpu.VMEM)
    rows, angles, lanes = rising.shape
    shape = jax.ShapeDtypeStruct((rows // quarters, angles, lanes), jnp.bfloat16)
    return pl.pallas_call(
        total_kernel,
        out_shape=(shape,) * quarters,
        in_specs=[pl.BlockSpec(memory_space=pltpu.SMEM), vmem, vmem, vmem, vmem],
        out_specs=(vmem,) * quarters,
        compiler_params=pltpu.CompilerParams(vmem_limit_bytes=8 * 2**20),
        cost_estimate=pl.CostEstimate(
            flops=500_000_000, bytes_accessed=2**20, transcendentals=0
        ),
        name="total",
    )(side, gain, own, rising, falling)


def moments_kernel(group, cut_ref, w_ref, in_ref, out_ref):
    step = pl.program_id(0)
    angles, lanes = out_ref.shape
    count, hh, depth = in_ref.shape

    @pl.when(step == 0)
    def _():
        out_ref[...] = jnp.zeros_like(out_ref)

    row = lax.broadcasted_iota(jnp.int32, (angles, lanes), 0)
    total = out_ref[...]
    for part in range(count // group):
        gathers = in_ref[part * group : (part + 1) * group].reshape(group * hh, depth)
        square = None
        for q in range(depth // lanes):
            product = jnp.dot(
                w_ref[...],
                gathers[:, q * lanes : (q + 1) * lanes],
                preferred_element_type=jnp.float32,
            )
            square = product * product if square is None else square + product * product
        for j in range(group):
            cut = cut_ref[step * count + part * group + j]
            total += jnp.where(row < cut, square[j * angles : (j + 1) * angles], 0.0)
    out_ref[...] = total


def moments(offsets, weights, live):
    positions, hh, depth = offsets.shape
    angles = live.shape[1]
    per = 16
    squares = pl.pallas_call(
        functools.partial(moments_kernel, weights.shape[0] // angles),
        grid=(positions // per,),
        out_shape=jax.ShapeDtypeStruct((angles, LANES), jnp.float32),
        in_specs=[
            pl.BlockSpec(memory_space=pltpu.SMEM),
            pl.BlockSpec(weights.shape, lambda i: (0, 0)),
            pl.BlockSpec((per, hh, depth), lambda i: (i, 0, 0)),
        ],
        out_specs=pl.BlockSpec((angles, LANES), lambda i: (0, 0)),
        compiler_params=pltpu.CompilerParams(vmem_limit_bytes=60 * 2**20),
        cost_estimate=pl.CostEstimate(
            flops=10_000_000_000, bytes_accessed=6 * 2**20, transcendentals=0
        ),
        name="moments",
    )(jnp.sum(live, axis=1), weights, offsets)
    return jnp.sum(squares, axis=1), jnp.sum(live, axis=0).astype(jnp.float32)


def finish_kernel(side_ref, *refs):
    out_ref = refs[-1]
    halves = (refs[: len(refs) // 2], refs[len(refs) // 2 : -1])
    angles, lanes = refs[0].shape[1:]
    for half, parts in enumerate(halves):
        for k, ref in enumerate(parts):
            quarter = (side_ref[0] - k + len(parts)) % len(parts)
            start = pl.multiple_of(quarter * lanes, lanes)
            out_ref[:, half * angles : (half + 1) * angles, pl.ds(start, lanes)] = ref[...]


def finish(side, first, second):
    images, angles, lanes = first[0].shape
    vmem = pl.BlockSpec(memory_space=pltpu.VMEM)
    return pl.pallas_call(
        finish_kernel,
        out_shape=jax.ShapeDtypeStruct((images, 2 * angles, len(first) * lanes), jnp.bfloat16),
        in_specs=[pl.BlockSpec(memory_space=pltpu.SMEM)] + [vmem] * (2 * len(first)),
        out_specs=vmem,
        compiler_params=pltpu.CompilerParams(vmem_limit_bytes=8 * 2**20),
        name="finish",
    )(side, *first, *second)


def work(offsets, slant_weights, live, block_tile, image_slot):
    block_count = block_tile.shape[0]
    _, hh, depth = offsets.shape
    angles = slant_weights.shape[0]
    traces = 2 * angles
    size = 2 * hh
    tile_count = lax.axis_size(("shot_0", "shot_1", "shot_2"))
    columns = lax.axis_size(("shot_0", "shot_2"))
    quarters = lax.axis_size("grp")
    tile_rows = 4 * quarters
    blocks = offsets.reshape(block_count, size, depth)
    tiles = block_tile[:, 0]
    home = lax.axis_index("shot_1").reshape(1)

    def diagonal(count):
        return jnp.kron(jnp.eye(count, dtype=jnp.bfloat16), slant_weights)

    squares, counts = moments(offsets, diagonal(8), live)
    totals = jnp.concatenate([squares, counts])
    totals = lax.psum(totals, "shot_1")[None, :]

    pair = jnp.kron(jnp.eye(2 * CAP, dtype=jnp.bfloat16), slant_weights.T)

    def move(array, axis, shift):
        count = lax.axis_size(axis)
        return lax.ppermute(array, axis, [(i, (i + shift) % count) for i in range(count)])

    def packed(piece, **more):
        return pack(
            piece, home, tiles, image_slot, live.T, blocks,
            columns, quarters, tile_count, **more,
        )

    def exchange(sent):
        sent = sent.reshape((columns * quarters,) + sent.shape[2:])
        return lax.all_to_all(sent, PLANE, 0, 0, tiled=True)

    arrived = exchange(packed(FAR)[0])
    near = packed((FAR[1], RING - 1), groups=2)
    above = move(near[0], "shot_1", 1)
    below = move(near[1], "shot_1", -1)
    totals, pair = lax.optimization_barrier((totals, pair))
    own_piece = packed((RING - 1, RING), carried=(totals,), moved=(above, below))
    beside = exchange(own_piece[0])
    near_rows = 3 * CAP * size
    low = near_rows + CAP
    totals = jnp.sum(beside[:, low : low + 3].astype(jnp.float32), axis=(0, 1))
    gain = lax.rsqrt(totals[:angles] / (depth * totals[angles:]) + 1e-06)
    far_code = codes(arrived, FAR[1] * CAP * size, tile_rows)

    def stacked(shift, count):
        return stack(
            far_code, pair, arrived, shift, count, CAP, False,
            tile_rows, traces, jnp.bfloat16,
        )

    far = stacked(0, 1)
    rising = [move(far[0][0], "shot_1", 1), None]
    falling = [None, move(far[1][0], "shot_1", -1)]
    for n, shift in ((2, 1), (3, 3)):
        parts = stacked(shift, 2)
        for half in range(2):
            for chain, at, way in ((rising, 0, 1), (falling, 1, -1)):
                if chain[half] is None:
                    chain[half] = parts[half][at]
                else:
                    chain[half] = join(chain[half], parts[half], at)
                hops = way * (2 if n == 3 else 1)
                chain[half] = move(chain[half], "shot_1", hops)
    own = stack(
        codes(beside, near_rows, tile_rows), pair, beside, 0, 3,
        (beside.shape[1] - near_rows) // 3, True, tile_rows, traces, jnp.bfloat16,
    )
    side = lax.axis_index("grp").reshape(1)
    scale = jnp.broadcast_to(gain[:, None], (angles, LANES))
    ends = []
    for half in range(2):
        parts = total(side, scale, own[half], rising[half], falling[half], quarters)
        ends.append([parts[0]] + [move(parts[k], "grp", k) for k in range(1, quarters)])
    return finish(side, *ends)


def solution(mesh):
    torus = Mesh(
        mesh.devices.reshape(4, RING, 2, mesh.shape["grp"]),
        ("shot_0", "shot_1", "shot_2", "grp"),
    )
    return jax.shard_map(
        work,
        mesh=torus,
        in_specs=(P(SHOT_GRP, None, None), P(), P(SHOT_GRP, None), P(SHOT_GRP, None), P(SHOT_GRP)),
        out_specs=P(SHOT_GRP, None, None),
        check_vma=False,
    )
```

```python
import functools

import jax
import jax.numpy as jnp
from jax import lax
from jax.experimental import pallas as pl
from jax.experimental.pallas import tpu as pltpu
from jax.sharding import Mesh
from jax.sharding import PartitionSpec as P


SHOT_GRP = ("shot_0", "shot_1", "shot_2", "grp")
PLANE = ("shot_0", "shot_2", "grp")
RING = 8
LANES = 128
CAP = 2
FAR = (0, 5)


def pack_kernel(
    first, last, groups, carry, moved, home_ref, tile_ref, slot_ref, live_ref, off_ref, *refs
):
    total_ref, moved_refs = refs[:carry], refs[carry : carry + moved]
    out_refs = refs[carry + moved : carry + moved + groups]
    data, zeros, flags, meta, meta_low, count, goal = refs[carry + moved + groups :][:7]
    in_sems, out_sem, meta_sem, moved_sem = refs[-4:]
    blocks, size, _ = off_ref.shape
    positions = flags.shape[0]
    quarters = data.shape[0]
    tiles = count.shape[0]
    slots = (last - first) // groups * CAP
    columns = out_refs[0].shape[0]
    meta_at = slots * size * (1 + moved)
    meta_rows = meta.shape[1]
    parts = in_sems.shape[0]
    step = blocks // parts
    home = home_ref[0]

    def load(g, q):
        return pltpu.make_async_copy(
            off_ref.at[pl.ds(g * step, step), :, pl.ds(q * LANES, LANES)],
            data.at[q, pl.ds(g * step, step)],
            in_sems.at[g],
        )

    for g in range(parts):
        for q in range(quarters):
            load(g, q).start()

    def pass_on(m):
        rows = slots * size
        moves = (
            (0, (m + 1) * rows, rows),
            (rows, meta_at + (m + 1) * meta_rows, meta_rows),
        )
        return [
            pltpu.make_async_copy(
                moved_refs[m].at[:, :, pl.ds(source, length), :],
                out_refs[0].at[:, :, pl.ds(goal_row, length), :],
                moved_sem.at[2 * m + n],
            )
            for n, (source, goal_row, length) in enumerate(moves)
        ]

    for m in range(moved):
        for copy in pass_on(m):
            copy.start()
    zeros[...] = jnp.zeros_like(zeros)
    meta[...] = jnp.zeros_like(meta)

    def clear(t, _):
        count[t] = 0
        return 0

    lax.fori_loop(0, tiles, clear, 0, unroll=8)
    live = live_ref[...].astype(jnp.float32)
    twice = jnp.concatenate([live, live], axis=0)
    for low in range(0, positions, LANES):
        high = min(low + LANES, positions)
        turned = twice[:, low:high].T
        odd = lax.broadcasted_iota(jnp.int32, turned.shape, 0) % 2 == 1
        upper = lax.broadcasted_iota(jnp.int32, turned.shape, 1) >= LANES // 2
        flags[low:high, :] = jnp.where(odd == upper, turned, 0.0)

    def place(tile):
        ahead = ((tile // 2) % RING - home + RING) % RING
        near = jnp.minimum(ahead, RING - ahead)
        order = jnp.maximum(7 - 2 * near + (ahead > RING // 2).astype(jnp.int32), 0)
        column = (tile // (2 * RING)) * 2 + tile % 2
        mine = (order >= first) & (order < last)
        if groups > 1:
            return (order - first) * columns + column, 0, mine
        return column, (order - first) * CAP, mine

    def start(source, line, slot):
        rows = pl.ds(pl.multiple_of(slot * size, size), size)
        for k, out_ref in enumerate(out_refs):
            if groups == 1:
                target = out_ref.at[line, :, rows, :]
                pltpu.make_async_copy(source, target, out_sem).start()
            else:

                @pl.when((line >= k * columns) & (line < (k + 1) * columns))
                def _():
                    target = out_ref.at[line - k * columns, :, rows, :]
                    pltpu.make_async_copy(source, target, out_sem).start()

    def plan(b, _):
        tile = tile_ref[b]
        rank = count[tile]
        count[tile] = rank + 1
        column, slot, mine = place(tile)
        goal[b] = jnp.where(mine, column * 64 + slot + rank, -1)

        @pl.when(mine)
        def _():
            mark = (slot_ref[b] + 1).astype(jnp.float32)
            row = flags[pl.ds(2 * b, 1), :] + flags[pl.ds(2 * b + 1, 1), :]
            meta[column, pl.ds(slot + rank, 1), :] = row * mark

        return 0

    lax.fori_loop(0, blocks, plan, 0, unroll=4)

    def fill(tile, _):
        used = count[tile]
        column, slot, mine = place(tile)
        for rank in range(CAP):

            @pl.when(mine & (used <= rank))
            def _():
                start(zeros, column, slot + rank)

        return 0

    lax.fori_loop(0, tiles, fill, 0, unroll=4)
    if total_ref:
        rest = total_ref[0][...]
        for term in range(3):
            part = rest.astype(jnp.bfloat16).astype(jnp.float32)
            rest = rest - part
            for column in range(meta.shape[0]):
                meta[column, slots + term : slots + term + 1, :] = part
    meta_low[...] = meta[...].astype(jnp.bfloat16)

    def send(b, _):
        at = goal[b]

        @pl.when(at >= 0)
        def _():
            start(data.at[:, b], at >> 6, at & 63)

        return 0

    def meta_copies():
        return [
            pltpu.make_async_copy(
                meta_low.at[pl.ds(k * columns, columns)],
                out_ref.at[:, q, pl.ds(meta_at, meta_rows), :],
                meta_sem,
            )
            for k, out_ref in enumerate(out_refs)
            for q in range(quarters)
        ]

    for g in range(parts):
        for q in range(quarters):
            load(g, q).wait()
        lax.fori_loop(g * step, (g + 1) * step, send, 0, unroll=4)
        if g == parts // 2:
            for copy in meta_copies():
                copy.start()
    for out_ref in out_refs:
        whole = out_ref.at[:, :, pl.ds(0, slots * size), :]
        pltpu.make_async_copy(whole, whole, out_sem).wait()
    for copy in meta_copies():
        copy.wait()
    for m in range(moved):
        for copy in pass_on(m):
            copy.wait()


def pack(
    piece, home, tiles, slots, live, blocks, columns, quarters, tile_count,
    groups=1, carried=(), moved=(),
):
    first, last = piece
    count, size, _ = blocks.shape
    rows = (last - first) // groups * CAP
    meta_rows = -(-(rows + 3 * len(carried)) // 8) * 8
    length = (rows * size + meta_rows) * (1 + len(moved))
    parts = 8
    vmem = pl.BlockSpec(memory_space=pltpu.VMEM)
    hbm = pl.BlockSpec(memory_space=pltpu.HBM)
    smem = pl.BlockSpec(memory_space=pltpu.SMEM)
    shape = jax.ShapeDtypeStruct((columns, quarters, length, LANES), jnp.bfloat16)
    return pl.pallas_call(
        functools.partial(pack_kernel, first, last, groups, len(carried), len(moved)),
        out_shape=(shape,) * groups,
        in_specs=[smem, smem, smem, vmem, hbm] + [vmem] * (len(carried) + len(moved)),
        out_specs=(hbm,) * groups,
        scratch_shapes=[
            pltpu.VMEM((quarters, count, size, LANES), jnp.bfloat16),
            pltpu.VMEM((quarters, size, LANES), jnp.bfloat16),
            pltpu.VMEM((2 * count, LANES), jnp.float32),
            pltpu.VMEM((groups * columns, meta_rows, LANES), jnp.float32),
            pltpu.VMEM((groups * columns, meta_rows, LANES), jnp.bfloat16),
            pltpu.SMEM((tile_count,), jnp.int32),
            pltpu.SMEM((count,), jnp.int32),
            pltpu.SemaphoreType.DMA((parts,)),
            pltpu.SemaphoreType.DMA,
            pltpu.SemaphoreType.DMA,
            pltpu.SemaphoreType.DMA((max(2 * len(moved), 1),)),
        ],
        compiler_params=pltpu.CompilerParams(
            vmem_limit_bytes=62 * 2**20
        ),
        cost_estimate=pl.CostEstimate(
            flops=8_000_000_000, bytes_accessed=10 * 2**20, transcendentals=0
        ),
    )(home, tiles, slots, live, blocks, *carried, *moved)


def stack_kernel(codes_each, stride, shift, merge, code_ref, w_ref, in_ref, first_ref, second_ref, acc):
    place, step = pl.program_id(0), pl.program_id(1)
    per = in_ref.shape[0]
    traces, lanes = acc.shape[1:]
    angles = traces // 2
    begins, ends = step == 0, step == pl.num_programs(1) - 1
    if merge:
        begins = begins & (place == 0)
        ends = ends & (place == pl.num_programs(0) - 1)

    @pl.when(begins)
    def _():
        acc[...] = jnp.zeros_like(acc)

    weights = w_ref[...].T
    row = lax.broadcasted_iota(jnp.int32, (angles, lanes), 0)
    for u in range(per):
        product = jnp.dot(weights, in_ref[u], preferred_element_type=jnp.float32)
        for j in range(CAP):
            code = code_ref[(step * per + u) * codes_each + (shift + place) * stride + j]
            label = code >> 14
            for half, cut in enumerate(((code >> 7) & 127, code & 127)):
                low = half * angles
                angle = product[j * traces + low : j * traces + low + angles]
                acc[label, low : low + angles, :] += jnp.where(row < cut, angle, 0.0)

    @pl.when(ends)
    def _():
        images = first_ref.shape[1]
        first_ref[0] = acc[:images, :angles].astype(first_ref.dtype)
        second_ref[0] = acc[:images, angles:].astype(second_ref.dtype)


def codes(arrived, rows, tile_rows):
    flags = arrived[:, rows:].astype(jnp.int32)
    lane = lax.broadcasted_iota(jnp.int32, flags.shape, 2)
    live = (flags > 0).astype(jnp.int32) * jnp.where(lane < LANES // 2, 128, 1)
    label = jnp.where(flags > 0, flags - 1, tile_rows) * 16384
    return jnp.sum(live + jnp.where(lane == 0, label, 0), axis=2).reshape(-1)


def stack(code, weights, arrived, shift, count, stride, merge, tile_rows, traces, dtype):
    sources, _, lanes = arrived.shape
    codes_each = code.shape[0] // sources
    height = weights.shape[0]
    per = 16
    half = (tile_rows, traces // 2, lanes)
    shape = jax.ShapeDtypeStruct((1 if merge else count,) + half, dtype)
    spec = pl.BlockSpec((1,) + half, lambda d, i: (0 if merge else d, 0, 0, 0))
    return pl.pallas_call(
        functools.partial(stack_kernel, codes_each, stride, shift, merge),
        grid=(count, sources // per),
        out_shape=(shape, shape),
        in_specs=[
            pl.BlockSpec(memory_space=pltpu.SMEM),
            pl.BlockSpec(weights.shape, lambda d, i: (0, 0)),
            pl.BlockSpec((per, height, lanes), lambda d, i: (i, shift + d, 0)),
        ],
        out_specs=(spec, spec),
        scratch_shapes=[pltpu.VMEM((tile_rows + 1, traces, lanes), jnp.float32)],
        compiler_params=pltpu.CompilerParams(
            vmem_limit_bytes=(44 if merge else 16) * 2**20
        ),
        cost_estimate=pl.CostEstimate(
            flops=2_500_000_000 * count, bytes_accessed=2**21 * count, transcendentals=0
        ),
    )(code, weights, arrived)


def join_kernel(at, passed_ref, own_ref, out_ref):
    value = passed_ref[...].astype(jnp.float32) + own_ref[at].astype(jnp.float32)
    out_ref[...] = value.astype(out_ref.dtype)


def join(passed, own, at):
    vmem = pl.BlockSpec(memory_space=pltpu.VMEM)
    return pl.pallas_call(
        functools.partial(join_kernel, at),
        out_shape=jax.ShapeDtypeStruct(passed.shape, passed.dtype),
        in_specs=[vmem, vmem],
        out_specs=vmem,
        compiler_params=pltpu.CompilerParams(vmem_limit_bytes=8 * 2**20),
        cost_estimate=pl.CostEstimate(
            flops=500_000_000, bytes_accessed=2**20, transcendentals=0
        ),
        name="join",
    )(passed, own)


def total_kernel(side_ref, gain_ref, *refs):
    own, rising, falling, out_refs = refs[0:2], refs[2:4], refs[4:6], refs[6:]
    images = out_refs[0].shape[0]
    gain = gain_ref[...]
    angles = gain.shape[0]
    for k, out_ref in enumerate(out_refs):
        start = (side_ref[0] + k) % len(out_refs) * images
        for i in range(images):
            for half in range(2):
                value = own[half][0, start + i].astype(jnp.float32)
                value = value + rising[half][start + i].astype(jnp.float32)
                value = (value + falling[half][start + i].astype(jnp.float32)) * gain
                low = half * angles
                out_ref[i, low : low + angles] = value.astype(out_ref.dtype)


def total(side, gain, own, rising, falling, quarters):
    vmem = pl.BlockSpec(memory_space=pltpu.VMEM)
    rows, angles, lanes = rising[0].shape
    shape = jax.ShapeDtypeStruct((rows // quarters, 2 * angles, lanes), jnp.bfloat16)
    return pl.pallas_call(
        total_kernel,
        out_shape=(shape,) * quarters,
        in_specs=[pl.BlockSpec(memory_space=pltpu.SMEM)] + [vmem] * 7,
        out_specs=(vmem,) * quarters,
        compiler_params=pltpu.CompilerParams(vmem_limit_bytes=8 * 2**20),
        cost_estimate=pl.CostEstimate(
            flops=500_000_000, bytes_accessed=2 * 2**20, transcendentals=0
        ),
        name="total",
    )(side, gain, *own, *rising, *falling)


def moments_kernel(group, cut_ref, w_ref, in_ref, out_ref):
    step = pl.program_id(0)
    angles, lanes = out_ref.shape
    count, hh, depth = in_ref.shape

    @pl.when(step == 0)
    def _():
        out_ref[...] = jnp.zeros_like(out_ref)

    row = lax.broadcasted_iota(jnp.int32, (angles, lanes), 0)
    total = out_ref[...]
    for part in range(count // group):
        gathers = in_ref[part * group : (part + 1) * group].reshape(group * hh, depth)
        square = None
        for q in range(depth // lanes):
            product = jnp.dot(
                w_ref[...],
                gathers[:, q * lanes : (q + 1) * lanes],
                preferred_element_type=jnp.float32,
            )
            square = product * product if square is None else square + product * product
        for j in range(group):
            cut = cut_ref[step * count + part * group + j]
            total += jnp.where(row < cut, square[j * angles : (j + 1) * angles], 0.0)
    out_ref[...] = total


def moments(offsets, weights, live):
    positions, hh, depth = offsets.shape
    angles = live.shape[1]
    per = 16
    squares = pl.pallas_call(
        functools.partial(moments_kernel, weights.shape[0] // angles),
        grid=(positions // per,),
        out_shape=jax.ShapeDtypeStruct((angles, LANES), jnp.float32),
        in_specs=[
            pl.BlockSpec(memory_space=pltpu.SMEM),
            pl.BlockSpec(weights.shape, lambda i: (0, 0)),
            pl.BlockSpec((per, hh, depth), lambda i: (i, 0, 0)),
        ],
        out_specs=pl.BlockSpec((angles, LANES), lambda i: (0, 0)),
        compiler_params=pltpu.CompilerParams(vmem_limit_bytes=60 * 2**20),
        cost_estimate=pl.CostEstimate(
            flops=10_000_000_000, bytes_accessed=6 * 2**20, transcendentals=0
        ),
        name="moments",
    )(jnp.sum(live, axis=1), weights, offsets)
    return jnp.sum(squares, axis=1), jnp.sum(live, axis=0).astype(jnp.float32)


def finish_kernel(side_ref, *refs):
    out_ref, parts = refs[-1], refs[:-1]
    lanes = parts[0].shape[2]
    for k, ref in enumerate(parts):
        quarter = (side_ref[0] - k + len(parts)) % len(parts)
        start = pl.multiple_of(quarter * lanes, lanes)
        out_ref[:, :, pl.ds(start, lanes)] = ref[...]


def finish(side, parts):
    images, traces, lanes = parts[0].shape
    vmem = pl.BlockSpec(memory_space=pltpu.VMEM)
    return pl.pallas_call(
        finish_kernel,
        out_shape=jax.ShapeDtypeStruct((images, traces, len(parts) * lanes), jnp.bfloat16),
        in_specs=[pl.BlockSpec(memory_space=pltpu.SMEM)] + [vmem] * len(parts),
        out_specs=vmem,
        compiler_params=pltpu.CompilerParams(vmem_limit_bytes=8 * 2**20),
        name="finish",
    )(side, *parts)


def work(offsets, slant_weights, live, block_tile, image_slot):
    block_count = block_tile.shape[0]
    _, hh, depth = offsets.shape
    angles = slant_weights.shape[0]
    traces = 2 * angles
    size = 2 * hh
    tile_count = lax.axis_size(("shot_0", "shot_1", "shot_2"))
    columns = lax.axis_size(("shot_0", "shot_2"))
    quarters = lax.axis_size("grp")
    tile_rows = 4 * quarters
    blocks = offsets.reshape(block_count, size, depth)
    tiles = block_tile[:, 0]
    home = lax.axis_index("shot_1").reshape(1)

    def diagonal(count):
        return jnp.kron(jnp.eye(count, dtype=jnp.bfloat16), slant_weights)

    squares, counts = moments(offsets, diagonal(8), live)
    totals = jnp.concatenate([squares, counts])
    totals = lax.psum(totals, "shot_1")[None, :]

    pair = jnp.kron(jnp.eye(2 * CAP, dtype=jnp.bfloat16), slant_weights.T)

    def move(array, axis, shift):
        count = lax.axis_size(axis)
        return lax.ppermute(array, axis, [(i, (i + shift) % count) for i in range(count)])

    def packed(piece, **more):
        return pack(
            piece, home, tiles, image_slot, live.T, blocks,
            columns, quarters, tile_count, **more,
        )

    def exchange(sent):
        sent = sent.reshape((columns * quarters,) + sent.shape[2:])
        return lax.all_to_all(sent, PLANE, 0, 0, tiled=True)

    arrived = exchange(packed(FAR)[0])
    near = packed((FAR[1], RING - 1), groups=2)
    above = move(near[0], "shot_1", 1)
    below = move(near[1], "shot_1", -1)
    totals, pair = lax.optimization_barrier((totals, pair))
    own_piece = packed((RING - 1, RING), carried=(totals,), moved=(above, below))
    beside = exchange(own_piece[0])
    near_rows = 3 * CAP * size
    low = near_rows + CAP
    totals = jnp.sum(beside[:, low : low + 3].astype(jnp.float32), axis=(0, 1))
    gain = lax.rsqrt(totals[:angles] / (depth * totals[angles:]) + 1e-06)
    far_code = codes(arrived, FAR[1] * CAP * size, tile_rows)

    def stacked(shift, count):
        return stack(
            far_code, pair, arrived, shift, count, CAP, False,
            tile_rows, traces, jnp.bfloat16,
        )

    far = stacked(0, 1)
    rising = [move(far[0][0], "shot_1", 1), None]
    falling = [None, move(far[1][0], "shot_1", -1)]
    for n, shift in ((2, 1), (3, 3)):
        parts = stacked(shift, 2)
        for half in range(2):
            for chain, at, way in ((rising, 0, 1), (falling, 1, -1)):
                if chain[half] is None:
                    chain[half] = parts[half][at]
                else:
                    chain[half] = join(chain[half], parts[half], at)
                hops = way * (2 if n == 3 else 1)
                chain[half] = move(chain[half], "shot_1", hops)
    own = stack(
        codes(beside, near_rows, tile_rows), pair, beside, 0, 3,
        (beside.shape[1] - near_rows) // 3, True, tile_rows, traces, jnp.bfloat16,
    )
    side = lax.axis_index("grp").reshape(1)
    scale = jnp.broadcast_to(gain[:, None], (angles, LANES))
    parts = total(side, scale, own, rising, falling, quarters)
    ends = [parts[0]] + [move(parts[k], "grp", k) for k in range(1, quarters)]
    return finish(side, ends)


def solution(mesh):
    torus = Mesh(
        mesh.devices.reshape(4, RING, 2, mesh.shape["grp"]),
        ("shot_0", "shot_1", "shot_2", "grp"),
    )
    return jax.shard_map(
        work,
        mesh=torus,
        in_specs=(P(SHOT_GRP, None, None), P(), P(SHOT_GRP, None), P(SHOT_GRP, None), P(SHOT_GRP)),
        out_specs=P(SHOT_GRP, None, None),
        check_vma=False,
    )
```

```python
import functools

import jax
import jax.numpy as jnp
from jax import lax
from jax.experimental import pallas as pl
from jax.experimental.pallas import tpu as pltpu
from jax.sharding import Mesh
from jax.sharding import PartitionSpec as P


SHOT_GRP = ("shot_0", "shot_1", "shot_2", "grp")
PLANE = ("shot_0", "shot_2", "grp")
RING = 8
LANES = 128
CAP = 2
FAR = (0, 5)


def pack_kernel(
    first, last, groups, carry, moved, home_ref, tile_ref, slot_ref, live_ref, off_ref, *refs
):
    total_ref, moved_refs = refs[:carry], refs[carry : carry + moved]
    out_refs = refs[carry + moved : carry + moved + groups]
    data, zeros, flags, meta, meta_low, count, goal = refs[carry + moved + groups :][:7]
    in_sems, out_sem, meta_sem, moved_sem = refs[-4:]
    blocks, size, _ = off_ref.shape
    positions = flags.shape[0]
    quarters = data.shape[0]
    tiles = count.shape[0]
    slots = (last - first) // groups * CAP
    columns = out_refs[0].shape[0]
    meta_at = slots * size * (1 + moved)
    meta_rows = meta.shape[1]
    parts = in_sems.shape[0]
    step = blocks // parts
    home = home_ref[0]

    def load(g, q):
        return pltpu.make_async_copy(
            off_ref.at[pl.ds(g * step, step), :, pl.ds(q * LANES, LANES)],
            data.at[q, pl.ds(g * step, step)],
            in_sems.at[g],
        )

    for g in range(parts):
        for q in range(quarters):
            load(g, q).start()

    def pass_on(m):
        rows = slots * size
        moves = (
            (0, (m + 1) * rows, rows),
            (rows, meta_at + (m + 1) * meta_rows, meta_rows),
        )
        return [
            pltpu.make_async_copy(
                moved_refs[m].at[:, :, pl.ds(source, length), :],
                out_refs[0].at[:, :, pl.ds(goal_row, length), :],
                moved_sem.at[2 * m + n],
            )
            for n, (source, goal_row, length) in enumerate(moves)
        ]

    for m in range(moved):
        for copy in pass_on(m):
            copy.start()
    zeros[...] = jnp.zeros_like(zeros)
    meta[...] = jnp.zeros_like(meta)

    def clear(t, _):
        count[t] = 0
        return 0

    lax.fori_loop(0, tiles, clear, 0, unroll=8)
    live = live_ref[...].astype(jnp.float32)
    twice = jnp.concatenate([live, live], axis=0)
    for low in range(0, positions, LANES):
        high = min(low + LANES, positions)
        turned = twice[:, low:high].T
        odd = lax.broadcasted_iota(jnp.int32, turned.shape, 0) % 2 == 1
        upper = lax.broadcasted_iota(jnp.int32, turned.shape, 1) >= LANES // 2
        flags[low:high, :] = jnp.where(odd == upper, turned, 0.0)

    def place(tile):
        ahead = ((tile // 2) % RING - home + RING) % RING
        near = jnp.minimum(ahead, RING - ahead)
        order = jnp.maximum(7 - 2 * near + (ahead > RING // 2).astype(jnp.int32), 0)
        column = (tile // (2 * RING)) * 2 + tile % 2
        mine = (order >= first) & (order < last)
        if groups > 1:
            return (order - first) * columns + column, 0, mine
        return column, (order - first) * CAP, mine

    def start(source, line, slot):
        rows = pl.ds(pl.multiple_of(slot * size, size), size)
        for k, out_ref in enumerate(out_refs):
            if groups == 1:
                target = out_ref.at[line, :, rows, :]
                pltpu.make_async_copy(source, target, out_sem).start()
            else:

                @pl.when((line >= k * columns) & (line < (k + 1) * columns))
                def _():
                    target = out_ref.at[line - k * columns, :, rows, :]
                    pltpu.make_async_copy(source, target, out_sem).start()

    def plan(b, _):
        tile = tile_ref[b]
        rank = count[tile]
        count[tile] = rank + 1
        column, slot, mine = place(tile)
        goal[b] = jnp.where(mine, column * 64 + slot + rank, -1)

        @pl.when(mine)
        def _():
            mark = (slot_ref[b] + 1).astype(jnp.float32)
            row = flags[pl.ds(2 * b, 1), :] + flags[pl.ds(2 * b + 1, 1), :]
            meta[column, pl.ds(slot + rank, 1), :] = row * mark

        return 0

    lax.fori_loop(0, blocks, plan, 0, unroll=4)

    def fill(tile, _):
        used = count[tile]
        column, slot, mine = place(tile)
        for rank in range(CAP):

            @pl.when(mine & (used <= rank))
            def _():
                start(zeros, column, slot + rank)

        return 0

    lax.fori_loop(0, tiles, fill, 0, unroll=4)
    if total_ref:
        rest = total_ref[0][...]
        for term in range(3):
            part = rest.astype(jnp.bfloat16).astype(jnp.float32)
            rest = rest - part
            for column in range(meta.shape[0]):
                meta[column, slots + term : slots + term + 1, :] = part
    meta_low[...] = meta[...].astype(jnp.bfloat16)

    def send(b, _):
        at = goal[b]

        @pl.when(at >= 0)
        def _():
            start(data.at[:, b], at >> 6, at & 63)

        return 0

    def meta_copies():
        return [
            pltpu.make_async_copy(
                meta_low.at[pl.ds(k * columns, columns)],
                out_ref.at[:, q, pl.ds(meta_at, meta_rows), :],
                meta_sem,
            )
            for k, out_ref in enumerate(out_refs)
            for q in range(quarters)
        ]

    for g in range(parts):
        for q in range(quarters):
            load(g, q).wait()
        lax.fori_loop(g * step, (g + 1) * step, send, 0, unroll=4)
        if g == parts // 2:
            for copy in meta_copies():
                copy.start()
    for out_ref in out_refs:
        whole = out_ref.at[:, :, pl.ds(0, slots * size), :]
        pltpu.make_async_copy(whole, whole, out_sem).wait()
    for copy in meta_copies():
        copy.wait()
    for m in range(moved):
        for copy in pass_on(m):
            copy.wait()


def pack(
    piece, home, tiles, slots, live, blocks, columns, quarters, tile_count,
    groups=1, carried=(), moved=(),
):
    first, last = piece
    count, size, _ = blocks.shape
    rows = (last - first) // groups * CAP
    meta_rows = -(-(rows + 3 * len(carried)) // 8) * 8
    length = (rows * size + meta_rows) * (1 + len(moved))
    parts = 8
    vmem = pl.BlockSpec(memory_space=pltpu.VMEM)
    hbm = pl.BlockSpec(memory_space=pltpu.HBM)
    smem = pl.BlockSpec(memory_space=pltpu.SMEM)
    shape = jax.ShapeDtypeStruct((columns, quarters, length, LANES), jnp.bfloat16)
    return pl.pallas_call(
        functools.partial(pack_kernel, first, last, groups, len(carried), len(moved)),
        out_shape=(shape,) * groups,
        in_specs=[smem, smem, smem, vmem, hbm] + [vmem] * (len(carried) + len(moved)),
        out_specs=(hbm,) * groups,
        scratch_shapes=[
            pltpu.VMEM((quarters, count, size, LANES), jnp.bfloat16),
            pltpu.VMEM((quarters, size, LANES), jnp.bfloat16),
            pltpu.VMEM((2 * count, LANES), jnp.float32),
            pltpu.VMEM((groups * columns, meta_rows, LANES), jnp.float32),
            pltpu.VMEM((groups * columns, meta_rows, LANES), jnp.bfloat16),
            pltpu.SMEM((tile_count,), jnp.int32),
            pltpu.SMEM((count,), jnp.int32),
            pltpu.SemaphoreType.DMA((parts,)),
            pltpu.SemaphoreType.DMA,
            pltpu.SemaphoreType.DMA,
            pltpu.SemaphoreType.DMA((max(2 * len(moved), 1),)),
        ],
        compiler_params=pltpu.CompilerParams(
            vmem_limit_bytes=62 * 2**20
        ),
        cost_estimate=pl.CostEstimate(
            flops=8_000_000_000, bytes_accessed=10 * 2**20, transcendentals=0
        ),
    )(home, tiles, slots, live, blocks, *carried, *moved)


def stack_kernel(codes_each, stride, shift, merge, code_ref, w_ref, in_ref, first_ref, second_ref, acc):
    place, step = pl.program_id(0), pl.program_id(1)
    per = in_ref.shape[0]
    traces, lanes = acc.shape[1:]
    angles = traces // 2
    begins, ends = step == 0, step == pl.num_programs(1) - 1
    if merge:
        begins = begins & (place == 0)
        ends = ends & (place == pl.num_programs(0) - 1)

    @pl.when(begins)
    def _():
        acc[...] = jnp.zeros_like(acc)

    weights = w_ref[...].T
    row = lax.broadcasted_iota(jnp.int32, (angles, lanes), 0)
    for u in range(per):
        product = jnp.dot(weights, in_ref[u], preferred_element_type=jnp.float32)
        for j in range(CAP):
            code = code_ref[(step * per + u) * codes_each + (shift + place) * stride + j]
            label = code >> 14
            for half, cut in enumerate(((code >> 7) & 127, code & 127)):
                low = half * angles
                angle = product[j * traces + low : j * traces + low + angles]
                acc[label, low : low + angles, :] += jnp.where(row < cut, angle, 0.0)

    @pl.when(ends)
    def _():
        images = first_ref.shape[1]
        first_ref[0] = acc[:images, :angles].astype(first_ref.dtype)
        second_ref[0] = acc[:images, angles:].astype(second_ref.dtype)


def codes(arrived, rows, tile_rows):
    flags = arrived[:, rows:].astype(jnp.int32)
    lane = lax.broadcasted_iota(jnp.int32, flags.shape, 2)
    live = (flags > 0).astype(jnp.int32) * jnp.where(lane < LANES // 2, 128, 1)
    label = jnp.where(flags > 0, flags - 1, tile_rows) * 16384
    return jnp.sum(live + jnp.where(lane == 0, label, 0), axis=2).reshape(-1)


def stack(code, weights, arrived, shift, count, stride, merge, tile_rows, traces, dtype):
    sources, _, lanes = arrived.shape
    codes_each = code.shape[0] // sources
    height = weights.shape[0]
    per = 16
    half = (tile_rows, traces // 2, lanes)
    shape = jax.ShapeDtypeStruct((1 if merge else count,) + half, dtype)
    spec = pl.BlockSpec((1,) + half, lambda d, i: (0 if merge else d, 0, 0, 0))
    return pl.pallas_call(
        functools.partial(stack_kernel, codes_each, stride, shift, merge),
        grid=(count, sources // per),
        out_shape=(shape, shape),
        in_specs=[
            pl.BlockSpec(memory_space=pltpu.SMEM),
            pl.BlockSpec(weights.shape, lambda d, i: (0, 0)),
            pl.BlockSpec((per, height, lanes), lambda d, i: (i, shift + d, 0)),
        ],
        out_specs=(spec, spec),
        scratch_shapes=[pltpu.VMEM((tile_rows + 1, traces, lanes), jnp.float32)],
        compiler_params=pltpu.CompilerParams(
            vmem_limit_bytes=(44 if merge else 16) * 2**20
        ),
        cost_estimate=pl.CostEstimate(
            flops=2_500_000_000 * count, bytes_accessed=2**21 * count, transcendentals=0
        ),
    )(code, weights, arrived)


def join_kernel(at, passed_ref, own_ref, out_ref):
    value = passed_ref[...].astype(jnp.float32) + own_ref[at].astype(jnp.float32)
    out_ref[...] = value.astype(out_ref.dtype)


def join(passed, own, at):
    vmem = pl.BlockSpec(memory_space=pltpu.VMEM)
    return pl.pallas_call(
        functools.partial(join_kernel, at),
        out_shape=jax.ShapeDtypeStruct(passed.shape, passed.dtype),
        in_specs=[vmem, vmem],
        out_specs=vmem,
        compiler_params=pltpu.CompilerParams(vmem_limit_bytes=8 * 2**20),
        cost_estimate=pl.CostEstimate(
            flops=500_000_000, bytes_accessed=2**20, transcendentals=0
        ),
        name="join",
    )(passed, own)


def total_kernel(ahead, quarters, side_ref, gain_ref, *refs):
    own, rising, falling, out_refs = refs[0:2], refs[2:4], refs[4:6], refs[6:]
    images = out_refs[0].shape[0]
    gain = gain_ref[...]
    angles = gain.shape[0]
    for k, out_ref in zip(ahead, out_refs):
        start = (side_ref[0] + k) % quarters * images
        for i in range(images):
            for half in range(2):
                value = own[half][0, start + i].astype(jnp.float32)
                value = value + rising[half][start + i].astype(jnp.float32)
                value = (value + falling[half][start + i].astype(jnp.float32)) * gain
                low = half * angles
                out_ref[i, low : low + angles] = value.astype(out_ref.dtype)


def total(ahead, side, gain, own, rising, falling, quarters):
    vmem = pl.BlockSpec(memory_space=pltpu.VMEM)
    rows, angles, lanes = rising[0].shape
    shape = jax.ShapeDtypeStruct((rows // quarters, 2 * angles, lanes), jnp.bfloat16)
    return pl.pallas_call(
        functools.partial(total_kernel, ahead, quarters),
        out_shape=(shape,) * len(ahead),
        in_specs=[pl.BlockSpec(memory_space=pltpu.SMEM)] + [vmem] * 7,
        out_specs=(vmem,) * len(ahead),
        compiler_params=pltpu.CompilerParams(vmem_limit_bytes=8 * 2**20),
        cost_estimate=pl.CostEstimate(
            flops=500_000_000, bytes_accessed=2 * 2**20, transcendentals=0
        ),
        name="total",
    )(side, gain, *own, *rising, *falling)


def moments_kernel(group, cut_ref, w_ref, in_ref, out_ref):
    step = pl.program_id(0)
    angles, lanes = out_ref.shape
    count, hh, depth = in_ref.shape

    @pl.when(step == 0)
    def _():
        out_ref[...] = jnp.zeros_like(out_ref)

    row = lax.broadcasted_iota(jnp.int32, (angles, lanes), 0)
    total = out_ref[...]
    for part in range(count // group):
        gathers = in_ref[part * group : (part + 1) * group].reshape(group * hh, depth)
        square = None
        for q in range(depth // lanes):
            product = jnp.dot(
                w_ref[...],
                gathers[:, q * lanes : (q + 1) * lanes],
                preferred_element_type=jnp.float32,
            )
            square = product * product if square is None else square + product * product
        for j in range(group):
            cut = cut_ref[step * count + part * group + j]
            total += jnp.where(row < cut, square[j * angles : (j + 1) * angles], 0.0)
    out_ref[...] = total


def moments(offsets, weights, live):
    positions, hh, depth = offsets.shape
    angles = live.shape[1]
    per = 16
    squares = pl.pallas_call(
        functools.partial(moments_kernel, weights.shape[0] // angles),
        grid=(positions // per,),
        out_shape=jax.ShapeDtypeStruct((angles, LANES), jnp.float32),
        in_specs=[
            pl.BlockSpec(memory_space=pltpu.SMEM),
            pl.BlockSpec(weights.shape, lambda i: (0, 0)),
            pl.BlockSpec((per, hh, depth), lambda i: (i, 0, 0)),
        ],
        out_specs=pl.BlockSpec((angles, LANES), lambda i: (0, 0)),
        compiler_params=pltpu.CompilerParams(vmem_limit_bytes=60 * 2**20),
        cost_estimate=pl.CostEstimate(
            flops=10_000_000_000, bytes_accessed=6 * 2**20, transcendentals=0
        ),
        name="moments",
    )(jnp.sum(live, axis=1), weights, offsets)
    return jnp.sum(squares, axis=1), jnp.sum(live, axis=0).astype(jnp.float32)


def finish_kernel(side_ref, *refs):
    out_ref, parts = refs[-1], refs[:-1]
    lanes = parts[0].shape[2]
    for k, ref in enumerate(parts):
        quarter = (side_ref[0] - k + len(parts)) % len(parts)
        start = pl.multiple_of(quarter * lanes, lanes)
        out_ref[:, :, pl.ds(start, lanes)] = ref[...]


def finish(side, parts):
    images, traces, lanes = parts[0].shape
    vmem = pl.BlockSpec(memory_space=pltpu.VMEM)
    return pl.pallas_call(
        finish_kernel,
        out_shape=jax.ShapeDtypeStruct((images, traces, len(parts) * lanes), jnp.bfloat16),
        in_specs=[pl.BlockSpec(memory_space=pltpu.SMEM)] + [vmem] * len(parts),
        out_specs=vmem,
        compiler_params=pltpu.CompilerParams(vmem_limit_bytes=8 * 2**20),
        name="finish",
    )(side, *parts)


def work(offsets, slant_weights, live, block_tile, image_slot):
    block_count = block_tile.shape[0]
    _, hh, depth = offsets.shape
    angles = slant_weights.shape[0]
    traces = 2 * angles
    size = 2 * hh
    tile_count = lax.axis_size(("shot_0", "shot_1", "shot_2"))
    columns = lax.axis_size(("shot_0", "shot_2"))
    quarters = lax.axis_size("grp")
    tile_rows = 4 * quarters
    blocks = offsets.reshape(block_count, size, depth)
    tiles = block_tile[:, 0]
    home = lax.axis_index("shot_1").reshape(1)

    def diagonal(count):
        return jnp.kron(jnp.eye(count, dtype=jnp.bfloat16), slant_weights)

    squares, counts = moments(offsets, diagonal(8), live)
    totals = jnp.concatenate([squares, counts])
    totals = lax.psum(totals, "shot_1")[None, :]

    pair = jnp.kron(jnp.eye(2 * CAP, dtype=jnp.bfloat16), slant_weights.T)

    def move(array, axis, shift):
        count = lax.axis_size(axis)
        return lax.ppermute(array, axis, [(i, (i + shift) % count) for i in range(count)])

    def packed(piece, **more):
        return pack(
            piece, home, tiles, image_slot, live.T, blocks,
            columns, quarters, tile_count, **more,
        )

    def exchange(sent):
        sent = sent.reshape((columns * quarters,) + sent.shape[2:])
        return lax.all_to_all(sent, PLANE, 0, 0, tiled=True)

    arrived = exchange(packed(FAR)[0])
    near = packed((FAR[1], RING - 1), groups=2)
    above = move(near[0], "shot_1", 1)
    below = move(near[1], "shot_1", -1)
    totals, pair = lax.optimization_barrier((totals, pair))
    own_piece = packed((RING - 1, RING), carried=(totals,), moved=(above, below))
    beside = exchange(own_piece[0])
    near_rows = 3 * CAP * size
    low = near_rows + CAP
    totals = jnp.sum(beside[:, low : low + 3].astype(jnp.float32), axis=(0, 1))
    gain = lax.rsqrt(totals[:angles] / (depth * totals[angles:]) + 1e-06)
    far_code = codes(arrived, FAR[1] * CAP * size, tile_rows)

    def stacked(shift, count):
        return stack(
            far_code, pair, arrived, shift, count, CAP, False,
            tile_rows, traces, jnp.bfloat16,
        )

    far = stacked(0, 1)
    rising = [move(far[0][0], "shot_1", 1), None]
    falling = [None, move(far[1][0], "shot_1", -1)]
    for n, shift in ((2, 1), (3, 3)):
        parts = stacked(shift, 2)
        for half in range(2):
            for chain, at, way in ((rising, 0, 1), (falling, 1, -1)):
                if chain[half] is None:
                    chain[half] = parts[half][at]
                else:
                    chain[half] = join(chain[half], parts[half], at)
                hops = way * (2 if n == 3 else 1)
                chain[half] = move(chain[half], "shot_1", hops)
    own = stack(
        codes(beside, near_rows, tile_rows), pair, beside, 0, 3,
        (beside.shape[1] - near_rows) // 3, True, tile_rows, traces, jnp.bfloat16,
    )
    side = lax.axis_index("grp").reshape(1)
    scale = jnp.broadcast_to(gain[:, None], (angles, LANES))
    away = tuple(range(1, quarters))
    parts = total(away, side, scale, own, rising, falling, quarters)
    ends = list(total((0,), side, scale, own, rising, falling, quarters))
    ends += [move(part, "grp", k) for k, part in zip(away, parts)]
    return finish(side, ends)


def solution(mesh):
    torus = Mesh(
        mesh.devices.reshape(4, RING, 2, mesh.shape["grp"]),
        ("shot_0", "shot_1", "shot_2", "grp"),
    )
    return jax.shard_map(
        work,
        mesh=torus,
        in_specs=(P(SHOT_GRP, None, None), P(), P(SHOT_GRP, None), P(SHOT_GRP, None), P(SHOT_GRP)),
        out_specs=P(SHOT_GRP, None, None),
        check_vma=False,
    )
```
